128 devices in a mesh: day: 16 (over x_lo, y, core), year: 8 (over z, x_hi).
Axes of the slice: x: 4 (x_hi: 2, x_lo: 2; x = x_hi * 2 + x_lo), y: 4, z: 4, core: 2. Of those that a mesh axis runs over, the one named last changes fastest.
Arguments:
- field: bfloat16 [32, 368, 2, 11520], P('year', 'day'), may hold values from -14 to 14
- day_index: int32 [32, 368], P('year', 'day'), may hold values from 0 to 367, as said below
- sample_count: int32 [32, 368, 2], P('year', 'day'), may hold values from 1 to 4
Outputs:
- anomaly: bfloat16 [32, 368, 2, 11520], P('year', 'day')
- climatology: bfloat16 [368, 2, 11520], P('day', None, 'year')
The draws below stay inside these ranges and needn't reach their ends.
Inputs may be any that keep to these rules, and one draw needn't show every extreme that they name: In each year either day_index[y, s] = s for every slot, or there is a slot from which on day_index[y, s] = (s + 1) mod 368 and before which day_index[y, s] = s.
All inputs are finite; a program needn't handle non-finite values.
Results may differ from the reference program's by a relative error of at most 0.001.
Values sent between devices are 32-bit elements; how exact they have to be, the bound alone decides.
A program may use at most 128 MiB of HBM per device.

```python
import math
import jax
import jax.numpy as jnp
from jax import lax

HOURS = 2
HALF = 30
DAYS = 368
YEARS = 32
CELLS = 11520


def calendar(key):
    inner = jax.random.fold_in(key, 11)
    first_key, second_key = jax.random.split(inner)
    leap_flag = jax.random.randint(first_key, (YEARS,), 0, 2)
    cut_slot = jax.random.randint(second_key, (YEARS,), 0, DAYS)
    slots = jnp.arange(DAYS, dtype=jnp.int32)[None, :]
    moved = (slots >= cut_slot[:, None]).astype(jnp.int32) * (1 - leap_flag[:, None])
    return jnp.mod(slots + moved, DAYS).astype(jnp.int32)


def draw_day_index(key, part):
    return calendar(key)


def draw_field(key, part):
    calendar_days = calendar(key)
    inner = jax.random.fold_in(key, 23)
    keys = jax.random.split(inner, 4)
    phase = jax.random.uniform(keys[0], (CELLS,), jnp.float32, 0.0, 2.0 * math.pi)
    amplitude = jax.random.uniform(keys[1], (HOURS, CELLS), jnp.float32, 1.0, 3.0)
    day_axis = jnp.arange(DAYS, dtype=jnp.float32)[:, None, None]
    season = amplitude[None] * jnp.cos(2.0 * math.pi * day_axis / DAYS + phase[None, None, :])
    rough = 0.8 * jnp.clip(jax.random.normal(keys[2], (DAYS, HOURS, CELLS), jnp.float32), -3.0, 3.0)
    base_field = season + rough
    noise = jnp.clip(jax.random.normal(keys[3], (YEARS, DAYS, HOURS, CELLS), jnp.float32), -4.0, 4.0)
    values = base_field[calendar_days] + noise
    return values.astype(jnp.bfloat16)


def place_ends(result, stream_key, low, largest):
    index_at = [jax.random.randint(jax.random.fold_in(stream_key, axis), (), 0, length) for axis, length in enumerate(result.shape)]
    longest = result.shape.index(max(result.shape))
    beside = index_at[:longest] + [(index_at[longest] + 1) % result.shape[longest]] + index_at[longest + 1:]
    return result.at[tuple(index_at)].set(low).at[tuple(beside)].set(largest)


def setup_inputs(seed: int = 0) -> dict:
    seeds = jax.random.split(jax.random.key(seed), 4)
    return {
        "field": draw_field(jax.random.fold_in(seeds[3], 71), 0),
        "day_index": draw_day_index(jax.random.fold_in(seeds[3], 71), 0),
        "sample_count": place_ends(jax.random.randint(seeds[2], (YEARS, DAYS, HOURS), 1, 5), jax.random.fold_in(seeds[2], 1), 1, 4).astype(jnp.int32),
    }


def reference(field, day_index, sample_count):
    weights = sample_count.astype(jnp.float32)

    def add_year(carry, inputs):
        rows, days, counts = inputs
        values = rows.astype(jnp.float32) * counts[:, :, None]
        sums = carry[0] + jax.ops.segment_sum(values, days, num_segments=DAYS)
        totals = carry[1] + jax.ops.segment_sum(counts, days, num_segments=DAYS)
        return (sums, totals), None

    initial = (jnp.zeros((DAYS, HOURS, CELLS), jnp.float32), jnp.zeros((DAYS, HOURS), jnp.float32))
    (day_sums, day_counts), _ = lax.scan(add_year, initial, (field, day_index, weights))
    window_sums = jnp.zeros((DAYS, HOURS, CELLS), jnp.float32)
    window_counts = jnp.zeros((DAYS, HOURS), jnp.float32)
    for offset in range(-HALF, HALF + 1):
        window_sums = window_sums + jnp.roll(day_sums, -offset, axis=0)
        window_counts = window_counts + jnp.roll(day_counts, -offset, axis=0)
    climate = window_sums / window_counts[:, :, None]

    def anomaly_year(inputs):
        rows, days = inputs
        return (rows.astype(jnp.float32) - climate[days]).astype(jnp.bfloat16)

    anomaly = lax.map(anomaly_year, (field, day_index))
    return anomaly, climate.astype(jnp.bfloat16)
```

```python
import functools

import jax
import jax.numpy as jnp
from jax import lax
from jax.experimental import pallas as pl
from jax.experimental.layout import Layout, with_layout_constraint
from jax.experimental.pallas import tpu as pltpu
from jax.sharding import PartitionSpec as P

MESH = pl.DeviceIdType.MESH
HALF = 30
YEARS, DAYS, HOURS, TILES = 4, 23, 2, 90
LANES = 128
ROWS = DAYS + 1
MID = ROWS // 2
SLOT, FIRST, SECOND = 23, 13, 10
SHARE, SKIP = 7, 6
MESSAGES = 64


def lanes(start, tiles):
    return pl.ds(pl.multiple_of(start * LANES, LANES), tiles * LANES)


def rows_of(low):
    return pl.ds(0, MID) if low else pl.ds(MID, MID)


def reduce_kernel(
    field, count_ref, index_ref, cl, held, part, weight, first_count, second_count,
    count0, count1, count2, count_x, count_z, count_d, first_in, second_in, second_x, first_x,
    first_share, second_share, first_win, second_win, kept, inverse, load_sem, send_sem, recv_sem,
):
    day = lax.axis_index("day")
    year = lax.axis_index("year")
    days = lax.axis_size("day")
    z, u = year // 2, year % 2
    up, down, across = (z + 1) % 4, (z + 3) % 4, (z + 2) % 4
    at_up, at_down, at_across = (day, up * 2 + u), (day, down * 2 + u), (day, across * 2 + u)
    twin = (day, z * 2 + (1 - u))
    beside = [((day + step + days) % days, year) for step in (1, -1, 2, -2)]
    peers = [at_up, at_down, at_across, twin] + beside

    barrier = pltpu.get_barrier_semaphore()
    for peer in peers:
        pl.semaphore_signal(barrier, inc=1, device_id=peer, device_id_type=MESH)

    pieces = [(0, 24), (24, 24), (48, 24), (72, 18)]
    loads = []
    for number, (start, tiles) in enumerate(pieces):
        span = pl.ds(start * LANES, tiles * LANES)
        load = pltpu.make_async_copy(
            field.at[:, :, :, span], held.at[:, :, :, span], load_sem.at[number]
        )
        load.start()
        loads.append(load)

    used = []

    def copy(source, target, device):
        number = len(used)
        used.append(
            pltpu.make_async_remote_copy(
                src_ref=source, dst_ref=target, send_sem=send_sem.at[number],
                recv_sem=recv_sem.at[number], device_id=device, device_id_type=MESH,
            )
        )
        used[-1].start()
        return used[-1]

    slot = lax.broadcasted_iota(jnp.int32, (YEARS, DAYS), 1) + day * DAYS
    moved = (index_ref[...] != slot).astype(jnp.float32)
    total_own = jnp.zeros((HOURS, DAYS), jnp.float32)
    total_next = jnp.zeros((HOURS, DAYS), jnp.float32)
    for y in range(YEARS):
        counts = count_ref[y].astype(jnp.float32)
        after = counts * moved[y : y + 1, :]
        own = counts - after
        total_own += own
        total_next += after
        for s in range(DAYS):
            weight[y, s] = jnp.broadcast_to(own[:, s : s + 1], (HOURS, 4 * LANES))
            weight[y, DAYS + s] = jnp.broadcast_to(after[:, s : s + 1], (HOURS, 4 * LANES))
    first_count[...] = jnp.zeros_like(first_count)
    second_count[...] = jnp.zeros_like(second_count)
    first_count[:, :DAYS] = total_own
    second_count[:, :DAYS] = total_next
    count0[...] = first_count[...] + pltpu.roll(second_count[...], 1, 1)

    def add_years(start, tiles):
        halves = [(h, min(4, tiles - h)) for h in range(0, tiles, 4)]
        carried = [None] * len(halves)
        for s in range(DAYS):
            own = [None] * len(halves)
            after = [None] * len(halves)
            for y in range(YEARS):
                value = held[y, s, :, lanes(start, tiles)].astype(jnp.float32)
                for n, (h, width) in enumerate(halves):
                    piece = value[:, h * LANES : (h + width) * LANES]
                    a = piece * weight[y, s, :, : width * LANES]
                    b = piece * weight[y, DAYS + s, :, : width * LANES]
                    own[n] = a if y == 0 else own[n] + a
                    after[n] = b if y == 0 else after[n] + b
            for n, (h, width) in enumerate(halves):
                row = own[n] if s == 0 else own[n] + carried[n]
                part[s, :, lanes(start + h, width)] = row
            carried = after
        for n, (h, width) in enumerate(halves):
            part[DAYS, :, lanes(start + h, width)] = carried[n]

    part[:, :, TILES * LANES :] = jnp.zeros((ROWS, HOURS, (4 * SLOT - TILES) * LANES), jnp.float32)
    for (start, tiles), load in zip(pieces, loads):
        load.wait()

        @pl.loop(0, tiles // 8)
        def _(step):
            add_years(start + step * 8, 8)

        if tiles % 8:
            add_years(start + tiles // 8 * 8, tiles % 8)

    pl.semaphore_wait(barrier, len(peers))

    def first_at(s):
        return s * SLOT

    def second_at(s):
        return s * SLOT + FIRST

    class Ring:
        def __init__(self, buffers, at, tiles):
            self.buffers, self.at, self.tiles = buffers, at, tiles

        def piece(self, low, s):
            return part.at[rows_of(low), :, lanes(self.at(s), self.tiles)]

        def begin(self):
            self.far_up = copy(self.piece(True, across), self.buffers.at[0], at_up)
            self.far_down = copy(self.piece(False, across), self.buffers.at[1], at_down)

        def near_up(self):
            self.up = copy(self.piece(False, up), self.buffers.at[2], at_up)

        def near_down(self):
            self.down = copy(self.piece(True, down), self.buffers.at[3], at_down)

        def forward(self):
            self.far_up.wait_recv()
            self.add(True, up, 0)
            self.on_up = copy(self.piece(True, up), self.buffers.at[4], at_up)
            self.far_down.wait_recv()
            self.add(False, down, 1)
            self.on_down = copy(self.piece(False, down), self.buffers.at[5], at_down)

        def add(self, low, s, number):
            where = (rows_of(low), slice(None), lanes(self.at(s), self.tiles))
            part[where] = part[where] + self.buffers[number]

        def result(self):
            self.up.wait_recv()
            self.down.wait_recv()
            self.on_up.wait_recv()
            self.on_down.wait_recv()
            where = lanes(self.at(z), self.tiles)
            low = part[rows_of(True), :, where] + self.buffers[3] + self.buffers[4]
            high = part[rows_of(False), :, where] + self.buffers[2] + self.buffers[5]
            return low, high

    first = Ring(first_in, first_at, FIRST)
    second = Ring(second_in, lambda s: second_at(s) + u * (SECOND // 2), SECOND // 2)

    send_count = copy(count0, count_x, twin)
    first.begin()
    swaps = []
    order = (across, up, down, z)
    for number, s in enumerate(order):
        source = part.at[:, :, lanes(second_at(s) + (1 - u) * (SECOND // 2), SECOND // 2)]
        swaps.append(copy(source, second_x.at[number], twin))
    first.near_up()
    first.near_down()

    def swapped(number):
        swaps[number].wait_recv()
        where = (slice(None), slice(None), lanes(second.at(order[number]), SECOND // 2))
        part[where] = part[where] + second_x[number]

    send_count.wait_recv()
    count1[...] = count0[...] + count_x[...]
    along = [copy(count1, count_z.at[n], d) for n, d in enumerate((at_up, at_down, at_across))]

    first.forward()
    swapped(0)
    second.begin()
    swapped(1)
    second.near_up()
    swapped(2)
    second.near_down()
    for message in along:
        message.wait_recv()
    count2[...] = count1[...] + count_z[0] + count_z[1] + count_z[2]
    aside = [copy(count2, count_d.at[n], d) for n, d in enumerate(beside)]
    second.forward()

    low, high = first.result()
    part[rows_of(True), :, lanes(first_at(z), FIRST)] = low
    part[rows_of(False), :, lanes(first_at(z), FIRST)] = high
    swap_first = copy(part.at[:, :, lanes(first_at(z) + (1 - u) * SKIP, SHARE)], first_x, twin)

    swapped(3)
    low, high = second.result()
    second_share[rows_of(True)] = low
    second_share[rows_of(False)] = high

    def share_out(share, window):
        right, left, right2, left2 = beside
        edge = ROWS // 3
        return [
            copy(share, window.at[pl.ds(0, ROWS)], right),
            copy(share, window.at[pl.ds(ROWS, ROWS)], left),
            copy(share.at[pl.ds(ROWS - edge, edge)], window.at[pl.ds(2 * ROWS, edge)], right2),
            copy(share.at[pl.ds(0, edge)], window.at[pl.ds(2 * ROWS + edge, edge)], left2),
        ]

    second_out = share_out(second_share, second_win)
    swap_first.wait_recv()
    first_share[...] = part[:, :, lanes(first_at(z) + u * SKIP, SHARE)] + first_x[...]
    first_out = share_out(first_share, first_win)

    for message in aside:
        message.wait_recv()
    spread = (
        count_d[2]
        + pltpu.roll(count_d[0], DAYS, 1)
        + pltpu.roll(count2[...], 2 * DAYS, 1)
        + pltpu.roll(count_d[1], 3 * DAYS, 1)
        + pltpu.roll(count_d[3], 4 * DAYS, 1)
    )
    lane = lax.broadcasted_iota(jnp.int32, (HOURS, LANES), 1)
    for i in range(ROWS):
        start = 2 * DAYS - HALF + i
        inside = (lane >= start) & (lane <= start + 2 * HALF)
        count = jnp.sum(jnp.where(inside, spread, 0.0), axis=1, keepdims=True)
        inverse[i] = jnp.broadcast_to(1.0 / count, (HOURS, 4 * LANES))

    def smooth(messages, share, window, at, tiles):
        for message in messages:
            message.wait_recv()
        edge = ROWS // 3

        def day_row(offset, span):
            def own(r):
                return share[r, :, span]

            def back(r):
                return window[r, :, span]

            def ahead(r):
                return window[ROWS + r, :, span]

            if offset < -DAYS:
                return window[2 * ROWS + offset + 2 * DAYS - (ROWS - edge), :, span]
            if offset == -DAYS:
                return back(0) + window[2 * ROWS + edge - 1, :, span]
            if offset < 0:
                return back(offset + DAYS)
            if offset == 0:
                return own(0) + back(DAYS)
            if offset < DAYS:
                return own(offset)
            if offset == DAYS:
                return ahead(0) + own(DAYS)
            if offset < 2 * DAYS:
                return ahead(offset - DAYS)
            if offset == 2 * DAYS:
                return window[2 * ROWS + edge, :, span] + ahead(DAYS)
            return window[2 * ROWS + edge + offset - 2 * DAYS, :, span]

        for h in range(0, tiles, 4):
            width = min(4, tiles - h)
            span = pl.ds(h * LANES, width * LANES)
            total = day_row(0, span)
            for offset in range(1, DAYS):
                total = total + day_row(offset, span)
            for offset in range(-1, -HALF - 1, -1):
                total = total + day_row(offset, span)
                if offset + HALF < ROWS:
                    kept[offset + HALF, :, : width * LANES] = total
            total = None
            for offset in range(DAYS, DAYS + HALF + 1):
                row = day_row(offset, span)
                total = row if total is None else total + row
                if offset >= HALF:
                    i = offset - HALF
                    sums = kept[i, :, : width * LANES] + total
                    cl[i, :, lanes(at + h, width)] = sums * inverse[i, :, : width * LANES]

    class Spread:
        def __init__(self, at, tiles):
            self.at, self.tiles = at, tiles

        def send(self, low, s, device):
            piece = cl.at[rows_of(low), :, lanes(self.at(s), self.tiles)]
            return copy(piece, piece, device)

        def begin(self):
            self.up0 = self.send(True, z, at_up)
            self.down0 = self.send(False, z, at_down)
            self.up1 = self.send(False, z, at_up)
            self.down1 = self.send(True, z, at_down)

        def forward(self):
            self.up0.wait_recv()
            self.up2 = self.send(True, down, at_up)
            self.down0.wait_recv()
            self.down2 = self.send(False, up, at_down)

        def near(self):
            self.up1.wait_recv()
            self.down1.wait_recv()

        def far(self):
            self.up2.wait_recv()
            self.down2.wait_recv()

    def across_x(s):
        piece = cl.at[:, :, lanes(second_at(s) + u * (SECOND // 2), SECOND // 2)]
        return copy(piece, piece, twin)

    second_spread = Spread(lambda s: second_at(s) + u * (SECOND // 2), SECOND // 2)
    own_spread = Spread(lambda s: first_at(s) + u * SKIP, SHARE)
    other_spread = Spread(lambda s: first_at(s) + (1 - u) * SHARE, SKIP)

    smooth(second_out, second_share, second_win, second_at(z) + u * (SECOND // 2), SECOND // 2)
    second_spread.begin()
    last = [across_x(z)]
    smooth(first_out, first_share, first_win, first_at(z) + u * SKIP, SHARE)
    piece = cl.at[:, :, lanes(first_at(z) + u * SHARE, SKIP)]
    to_twin = copy(piece, piece, twin)
    own_spread.begin()
    second_spread.forward()
    second_spread.near()
    last += [across_x(up), across_x(down)]
    to_twin.wait_recv()
    other_spread.begin()
    own_spread.forward()
    second_spread.far()
    last += [across_x(across)]
    other_spread.forward()
    for spread_portion in (own_spread, other_spread):
        spread_portion.near()
        spread_portion.far()
    for message in last:
        message.wait_recv()
    for message in used:
        message.wait_send()


def climate_of(field, day_index, counts):
    f32 = jnp.float32
    wide = 4 * SLOT * LANES
    vmem = pltpu.VMEM
    row = (HOURS, LANES)
    edge = ROWS // 3
    scratch = [
        vmem((YEARS, DAYS, HOURS, TILES * LANES), jnp.bfloat16),
        vmem((ROWS, HOURS, wide), f32),
        vmem((YEARS, 2 * DAYS, HOURS, 4 * LANES), f32),
        vmem(row, f32), vmem(row, f32), vmem(row, f32), vmem(row, f32), vmem(row, f32),
        vmem(row, f32), vmem((3, *row), f32), vmem((4, *row), f32),
        vmem((6, MID, HOURS, FIRST * LANES), f32),
        vmem((6, MID, HOURS, SECOND // 2 * LANES), f32),
        vmem((4, ROWS, HOURS, SECOND // 2 * LANES), f32),
        vmem((ROWS, HOURS, SHARE * LANES), f32),
        vmem((ROWS, HOURS, SHARE * LANES), f32),
        vmem((ROWS, HOURS, SECOND // 2 * LANES), f32),
        vmem((2 * ROWS + 2 * edge, HOURS, SHARE * LANES), f32),
        vmem((2 * ROWS + 2 * edge, HOURS, SECOND // 2 * LANES), f32),
        vmem((ROWS, HOURS, 4 * LANES), f32),
        vmem((ROWS, HOURS, 4 * LANES), f32),
        pltpu.SemaphoreType.DMA((4,)),
        pltpu.SemaphoreType.DMA((MESSAGES,)),
        pltpu.SemaphoreType.DMA((MESSAGES,)),
    ]
    return pl.pallas_call(
        reduce_kernel,
        out_shape=jax.ShapeDtypeStruct((ROWS, HOURS, wide), f32),
        in_specs=[
            pl.BlockSpec(memory_space=pl.ANY),
            pl.BlockSpec(memory_space=vmem),
            pl.BlockSpec(memory_space=vmem),
        ],
        out_specs=pl.BlockSpec(memory_space=vmem),
        scratch_shapes=scratch,
        compiler_params=pltpu.CompilerParams(
            collective_id=0, has_side_effects=True, vmem_limit_bytes=40 * 2**20
        ),
        name="climate",
    )(field, counts, day_index)


STRIP = HOURS * TILES
WIDE = HOURS * 4 * SLOT
PAIRS = YEARS * DAYS // 2
GROUP = 2


def subtract_kernel(index_ref, field, climate, out, moved_on, held, ready, load_sem, store_sem):
    day = lax.axis_index("day")
    size = GROUP * 2 * STRIP
    groups = PAIRS // GROUP
    loads = [
        pltpu.make_async_copy(
            field.at[pl.ds(g * size, size)], held.at[pl.ds(g * size, size)], load_sem.at[g]
        )
        for g in range(groups)
    ]
    for load in loads:
        load.start()

    @pl.loop(0, ROWS)
    def _(e):
        base = pl.multiple_of(e * (WIDE + 8), 8)
        value = climate[pl.ds(pl.multiple_of(e * WIDE, 8), STRIP), :]
        moved_on[pl.ds(base + 4, STRIP), :] = value

    sublane = lax.broadcasted_iota(jnp.int32, (8, LANES), 0)

    def row_of(k):
        y, s = divmod(k, DAYS)
        ahead = (index_ref[y, s] != day * DAYS + s).astype(jnp.int32)
        return s + ahead

    stores = []
    body = STRIP - STRIP % 8
    for g in range(groups):
        loads[g].wait()
        for pair in range(g * GROUP, (g + 1) * GROUP):
            start = pair * 2 * STRIP
            even = pl.multiple_of(row_of(2 * pair) * WIDE, 8)
            odd = pl.multiple_of(row_of(2 * pair + 1) * (WIDE + 8), 8)

            def put(offset, size, value):
                span = pl.ds(start + offset, size)
                ready[span, :] = (held[span, :].astype(jnp.float32) - value).astype(jnp.bfloat16)

            put(0, body, climate[pl.ds(even, body), :])
            middle = jnp.where(
                sublane < 4, climate[pl.ds(even + body, 8), :], moved_on[pl.ds(odd, 8), :]
            )
            put(body, 8, middle)
            put(body + 8, body, moved_on[pl.ds(odd + 8, body), :])
        store = pltpu.make_async_copy(
            ready.at[pl.ds(g * size, size)], out.at[pl.ds(g * size, size)], store_sem.at[g]
        )
        store.start()
        stores.append(store)
    for store in stores:
        store.wait()


def anomaly_of(field, day_index, climate):
    rows = YEARS * DAYS * STRIP
    groups = PAIRS // GROUP
    return pl.pallas_call(
        subtract_kernel,
        out_shape=jax.ShapeDtypeStruct((rows, LANES), jnp.bfloat16),
        in_specs=[
            pl.BlockSpec(memory_space=pltpu.SMEM),
            pl.BlockSpec(memory_space=pl.ANY),
            pl.BlockSpec(memory_space=pltpu.VMEM),
        ],
        out_specs=pl.BlockSpec(memory_space=pl.ANY),
        scratch_shapes=[
            pltpu.VMEM((ROWS * (WIDE + 8), LANES), jnp.float32),
            pltpu.VMEM((rows, LANES), jnp.bfloat16),
            pltpu.VMEM((rows, LANES), jnp.bfloat16),
            pltpu.SemaphoreType.DMA((groups,)),
            pltpu.SemaphoreType.DMA((groups,)),
        ],
        compiler_params=pltpu.CompilerParams(vmem_limit_bytes=40 * 2**20),
        name="anomaly",
    )(day_index, field, climate)


def tile_rows(array):
    *lead, hours, cells = array.shape
    tiles = cells // LANES
    split = array.reshape(-1, hours, tiles, LANES)
    split = with_layout_constraint(split, Layout(major_to_minor=(0, 2, 1, 3)))
    return split.transpose(0, 2, 1, 3).reshape(-1, LANES)


def from_tile_rows(rows, shape):
    *lead, hours, cells = shape
    tiles = cells // LANES
    split = rows.reshape(-1, tiles, hours, LANES).transpose(0, 2, 1, 3)
    split = with_layout_constraint(split, Layout(major_to_minor=(0, 2, 1, 3)))
    return split.reshape(shape)


def local(field, day_index, sample_count):
    climate = climate_of(field, day_index, jnp.transpose(sample_count, (0, 2, 1)))
    anomaly = anomaly_of(tile_rows(field), day_index, tile_rows(climate))
    anomaly = from_tile_rows(anomaly, field.shape)
    cells = TILES * LANES // lax.axis_size("year")
    share = lax.dynamic_slice(
        climate, (0, 0, lax.axis_index("year") * cells), (DAYS, HOURS, cells)
    )
    return anomaly, share.astype(jnp.bfloat16)


def solution(mesh):
    return jax.shard_map(
        local,
        mesh=mesh,
        in_specs=(P("year", "day", None, None), P("year", "day"), P("year", "day", None)),
        out_specs=(P("year", "day", None, None), P("day", None, "year")),
        check_vma=False,
    )
```

```python
import functools

import jax
import jax.numpy as jnp
from jax import lax
from jax.experimental import pallas as pl
from jax.experimental.layout import Layout, with_layout_constraint
from jax.experimental.pallas import tpu as pltpu
from jax.sharding import PartitionSpec as P

MESH = pl.DeviceIdType.MESH
HALF = 30
YEARS, DAYS, HOURS, TILES = 4, 23, 2, 90
LANES = 128
ROWS = DAYS + 1
MID = ROWS // 2
SLOT, FIRST, SECOND = 23, 13, 10
SHARE, SKIP = 7, 6
MESSAGES = 64


def lanes(start, tiles):
    return pl.ds(pl.multiple_of(start * LANES, LANES), tiles * LANES)


def rows_of(low):
    return pl.ds(0, MID) if low else pl.ds(MID, MID)


def reduce_kernel(
    field, count_ref, cl, held, part, weight, first_count, second_count,
    count0, count1, count2, count_x, count_z, count_d, first_in, second_in, second_x, first_x,
    first_share, second_share, first_win, second_win, kept, inverse, load_sem, send_sem, recv_sem,
):
    day = lax.axis_index("day")
    year = lax.axis_index("year")
    days = lax.axis_size("day")
    z, u = year // 2, year % 2
    up, down, across = (z + 1) % 4, (z + 3) % 4, (z + 2) % 4
    at_up, at_down, at_across = (day, up * 2 + u), (day, down * 2 + u), (day, across * 2 + u)
    twin = (day, z * 2 + (1 - u))
    beside = [((day + step + days) % days, year) for step in (1, -1, 2, -2)]
    peers = [at_up, at_down, at_across, twin] + beside

    barrier = pltpu.get_barrier_semaphore()
    for peer in peers:
        pl.semaphore_signal(barrier, inc=1, device_id=peer, device_id_type=MESH)

    pieces = [(0, 24), (24, 24), (48, 24), (72, 18)]
    loads = []
    for number, (start, tiles) in enumerate(pieces):
        span = pl.ds(start * LANES, tiles * LANES)
        load = pltpu.make_async_copy(
            field.at[:, :, :, span], held.at[:, :, :, span], load_sem.at[number]
        )
        load.start()
        loads.append(load)

    used = []

    def copy(source, target, device):
        number = len(used)
        used.append(
            pltpu.make_async_remote_copy(
                src_ref=source, dst_ref=target, send_sem=send_sem.at[number],
                recv_sem=recv_sem.at[number], device_id=device, device_id_type=MESH,
            )
        )
        used[-1].start()
        return used[-1]

    total_own = jnp.zeros((HOURS, DAYS), jnp.float32)
    total_next = jnp.zeros((HOURS, DAYS), jnp.float32)
    for y in range(YEARS):
        counts = count_ref[y].astype(jnp.float32)
        own = jnp.maximum(counts, 0.0)
        after = jnp.maximum(-counts, 0.0)
        total_own += own
        total_next += after
        for s in range(DAYS):
            weight[y, s] = jnp.broadcast_to(own[:, s : s + 1], (HOURS, 4 * LANES))
            weight[y, DAYS + s] = jnp.broadcast_to(after[:, s : s + 1], (HOURS, 4 * LANES))
    first_count[...] = jnp.zeros_like(first_count)
    second_count[...] = jnp.zeros_like(second_count)
    first_count[:, :DAYS] = total_own
    second_count[:, :DAYS] = total_next
    count0[...] = first_count[...] + pltpu.roll(second_count[...], 1, 1)

    def add_years(start, tiles):
        halves = [(h, min(4, tiles - h)) for h in range(0, tiles, 4)]
        carried = [None] * len(halves)
        for s in range(DAYS):
            own = [None] * len(halves)
            after = [None] * len(halves)
            for y in range(YEARS):
                value = held[y, s, :, lanes(start, tiles)].astype(jnp.float32)
                for n, (h, width) in enumerate(halves):
                    piece = value[:, h * LANES : (h + width) * LANES]
                    a = piece * weight[y, s, :, : width * LANES]
                    b = piece * weight[y, DAYS + s, :, : width * LANES]
                    own[n] = a if y == 0 else own[n] + a
                    after[n] = b if y == 0 else after[n] + b
            for n, (h, width) in enumerate(halves):
                row = own[n] if s == 0 else own[n] + carried[n]
                part[s, :, lanes(start + h, width)] = row
            carried = after
        for n, (h, width) in enumerate(halves):
            part[DAYS, :, lanes(start + h, width)] = carried[n]

    part[:, :, TILES * LANES :] = jnp.zeros((ROWS, HOURS, (4 * SLOT - TILES) * LANES), jnp.float32)
    for (start, tiles), load in zip(pieces, loads):
        load.wait()

        @pl.loop(0, tiles // 8)
        def _(step):
            add_years(start + step * 8, 8)

        if tiles % 8:
            add_years(start + tiles // 8 * 8, tiles % 8)

    pl.semaphore_wait(barrier, len(peers))

    def first_at(s):
        return s * SLOT

    def second_at(s):
        return s * SLOT + FIRST

    class Ring:
        def __init__(self, buffers, at, tiles):
            self.buffers, self.at, self.tiles = buffers, at, tiles

        def piece(self, low, s):
            return part.at[rows_of(low), :, lanes(self.at(s), self.tiles)]

        def begin(self):
            self.far_up = copy(self.piece(True, across), self.buffers.at[0], at_up)
            self.far_down = copy(self.piece(False, across), self.buffers.at[1], at_down)

        def near_up(self):
            self.up = copy(self.piece(False, up), self.buffers.at[2], at_up)

        def near_down(self):
            self.down = copy(self.piece(True, down), self.buffers.at[3], at_down)

        def forward(self):
            self.far_up.wait_recv()
            self.add(True, up, 0)
            self.on_up = copy(self.piece(True, up), self.buffers.at[4], at_up)
            self.far_down.wait_recv()
            self.add(False, down, 1)
            self.on_down = copy(self.piece(False, down), self.buffers.at[5], at_down)

        def add(self, low, s, number):
            where = (rows_of(low), slice(None), lanes(self.at(s), self.tiles))
            part[where] = part[where] + self.buffers[number]

        def result(self):
            self.up.wait_recv()
            self.down.wait_recv()
            self.on_up.wait_recv()
            self.on_down.wait_recv()
            where = lanes(self.at(z), self.tiles)
            low = part[rows_of(True), :, where] + self.buffers[3] + self.buffers[4]
            high = part[rows_of(False), :, where] + self.buffers[2] + self.buffers[5]
            return low, high

    first = Ring(first_in, first_at, FIRST)
    second = Ring(second_in, lambda s: second_at(s) + u * (SECOND // 2), SECOND // 2)

    send_count = copy(count0, count_x, twin)
    first.begin()
    swaps = []
    order = (across, up, down, z)
    for number, s in enumerate(order):
        source = part.at[:, :, lanes(second_at(s) + (1 - u) * (SECOND // 2), SECOND // 2)]
        swaps.append(copy(source, second_x.at[number], twin))
    first.near_up()
    first.near_down()

    def swapped(number):
        swaps[number].wait_recv()
        where = (slice(None), slice(None), lanes(second.at(order[number]), SECOND // 2))
        part[where] = part[where] + second_x[number]

    send_count.wait_recv()
    count1[...] = count0[...] + count_x[...]
    along = [copy(count1, count_z.at[n], d) for n, d in enumerate((at_up, at_down, at_across))]

    first.forward()
    swapped(0)
    second.begin()
    swapped(1)
    second.near_up()
    swapped(2)
    second.near_down()
    for message in along:
        message.wait_recv()
    count2[...] = count1[...] + count_z[0] + count_z[1] + count_z[2]
    aside = [copy(count2, count_d.at[n], d) for n, d in enumerate(beside)]
    second.forward()

    low, high = first.result()
    part[rows_of(True), :, lanes(first_at(z), FIRST)] = low
    part[rows_of(False), :, lanes(first_at(z), FIRST)] = high
    swap_first = copy(part.at[:, :, lanes(first_at(z) + (1 - u) * SKIP, SHARE)], first_x, twin)

    swapped(3)
    low, high = second.result()
    second_share[rows_of(True)] = low
    second_share[rows_of(False)] = high

    def share_out(share, window):
        right, left, right2, left2 = beside
        edge = ROWS // 3
        return [
            copy(share, window.at[pl.ds(0, ROWS)], right),
            copy(share, window.at[pl.ds(ROWS, ROWS)], left),
            copy(share.at[pl.ds(ROWS - edge, edge)], window.at[pl.ds(2 * ROWS, edge)], right2),
            copy(share.at[pl.ds(0, edge)], window.at[pl.ds(2 * ROWS + edge, edge)], left2),
        ]

    second_out = share_out(second_share, second_win)
    swap_first.wait_recv()
    first_share[...] = part[:, :, lanes(first_at(z) + u * SKIP, SHARE)] + first_x[...]
    first_out = share_out(first_share, first_win)

    for message in aside:
        message.wait_recv()
    spread = (
        count_d[2]
        + pltpu.roll(count_d[0], DAYS, 1)
        + pltpu.roll(count2[...], 2 * DAYS, 1)
        + pltpu.roll(count_d[1], 3 * DAYS, 1)
        + pltpu.roll(count_d[3], 4 * DAYS, 1)
    )
    lane = lax.broadcasted_iota(jnp.int32, (HOURS, LANES), 1)
    for i in range(ROWS):
        start = 2 * DAYS - HALF + i
        inside = (lane >= start) & (lane <= start + 2 * HALF)
        count = jnp.sum(jnp.where(inside, spread, 0.0), axis=1, keepdims=True)
        inverse[i] = jnp.broadcast_to(1.0 / count, (HOURS, 4 * LANES))

    def smooth(messages, share, window, at, tiles):
        for message in messages:
            message.wait_recv()
        edge = ROWS // 3

        def day_row(offset, span):
            def own(r):
                return share[r, :, span]

            def back(r):
                return window[r, :, span]

            def ahead(r):
                return window[ROWS + r, :, span]

            if offset < -DAYS:
                return window[2 * ROWS + offset + 2 * DAYS - (ROWS - edge), :, span]
            if offset == -DAYS:
                return back(0) + window[2 * ROWS + edge - 1, :, span]
            if offset < 0:
                return back(offset + DAYS)
            if offset == 0:
                return own(0) + back(DAYS)
            if offset < DAYS:
                return own(offset)
            if offset == DAYS:
                return ahead(0) + own(DAYS)
            if offset < 2 * DAYS:
                return ahead(offset - DAYS)
            if offset == 2 * DAYS:
                return window[2 * ROWS + edge, :, span] + ahead(DAYS)
            return window[2 * ROWS + edge + offset - 2 * DAYS, :, span]

        for h in range(0, tiles, 4):
            width = min(4, tiles - h)
            span = pl.ds(h * LANES, width * LANES)
            total = day_row(0, span)
            for offset in range(1, DAYS):
                total = total + day_row(offset, span)
            for offset in range(-1, -HALF - 1, -1):
                total = total + day_row(offset, span)
                if offset + HALF < ROWS:
                    kept[offset + HALF, :, : width * LANES] = total
            total = None
            for offset in range(DAYS, DAYS + HALF + 1):
                row = day_row(offset, span)
                total = row if total is None else total + row
                if offset >= HALF:
                    i = offset - HALF
                    sums = kept[i, :, : width * LANES] + total
                    cl[i, :, lanes(at + h, width)] = sums * inverse[i, :, : width * LANES]

    class Spread:
        def __init__(self, at, tiles):
            self.at, self.tiles = at, tiles

        def send(self, low, s, device):
            piece = cl.at[rows_of(low), :, lanes(self.at(s), self.tiles)]
            return copy(piece, piece, device)

        def begin(self):
            self.up0 = self.send(True, z, at_up)
            self.down0 = self.send(False, z, at_down)
            self.up1 = self.send(False, z, at_up)
            self.down1 = self.send(True, z, at_down)

        def forward(self):
            self.up0.wait_recv()
            self.up2 = self.send(True, down, at_up)
            self.down0.wait_recv()
            self.down2 = self.send(False, up, at_down)

        def near(self):
            self.up1.wait_recv()
            self.down1.wait_recv()

        def far(self):
            self.up2.wait_recv()
            self.down2.wait_recv()

    def across_x(s):
        piece = cl.at[:, :, lanes(second_at(s) + u * (SECOND // 2), SECOND // 2)]
        return copy(piece, piece, twin)

    second_spread = Spread(lambda s: second_at(s) + u * (SECOND // 2), SECOND // 2)
    own_spread = Spread(lambda s: first_at(s) + u * SKIP, SHARE)
    other_spread = Spread(lambda s: first_at(s) + (1 - u) * SHARE, SKIP)

    smooth(second_out, second_share, second_win, second_at(z) + u * (SECOND // 2), SECOND // 2)
    second_spread.begin()
    last = [across_x(z)]
    smooth(first_out, first_share, first_win, first_at(z) + u * SKIP, SHARE)
    piece = cl.at[:, :, lanes(first_at(z) + u * SHARE, SKIP)]
    to_twin = copy(piece, piece, twin)
    own_spread.begin()
    second_spread.forward()
    second_spread.near()
    last += [across_x(up), across_x(down)]
    to_twin.wait_recv()
    other_spread.begin()
    own_spread.forward()
    second_spread.far()
    last += [across_x(across)]
    other_spread.forward()
    for spread_portion in (own_spread, other_spread):
        spread_portion.near()
        spread_portion.far()
    for message in last:
        message.wait_recv()
    for message in used:
        message.wait_send()


def climate_of(field, counts):
    f32 = jnp.float32
    wide = 4 * SLOT * LANES
    vmem = pltpu.VMEM
    row = (HOURS, LANES)
    edge = ROWS // 3
    scratch = [
        vmem((ROWS, HOURS, wide), f32),
        vmem((YEARS, 2 * DAYS, HOURS, 4 * LANES), f32),
        vmem(row, f32), vmem(row, f32), vmem(row, f32), vmem(row, f32), vmem(row, f32),
        vmem(row, f32), vmem((3, *row), f32), vmem((4, *row), f32),
        vmem((6, MID, HOURS, FIRST * LANES), f32),
        vmem((6, MID, HOURS, SECOND // 2 * LANES), f32),
        vmem((4, ROWS, HOURS, SECOND // 2 * LANES), f32),
        vmem((ROWS, HOURS, SHARE * LANES), f32),
        vmem((ROWS, HOURS, SHARE * LANES), f32),
        vmem((ROWS, HOURS, SECOND // 2 * LANES), f32),
        vmem((2 * ROWS + 2 * edge, HOURS, SHARE * LANES), f32),
        vmem((2 * ROWS + 2 * edge, HOURS, SECOND // 2 * LANES), f32),
        vmem((ROWS, HOURS, 4 * LANES), f32),
        vmem((ROWS, HOURS, 4 * LANES), f32),
        pltpu.SemaphoreType.DMA((4,)),
        pltpu.SemaphoreType.DMA((MESSAGES,)),
        pltpu.SemaphoreType.DMA((MESSAGES,)),
    ]
    return pl.pallas_call(
        reduce_kernel,
        out_shape=(
            jax.ShapeDtypeStruct((ROWS, HOURS, wide), f32),
            jax.ShapeDtypeStruct(field.shape, field.dtype),
        ),
        in_specs=[
            pl.BlockSpec(memory_space=pltpu.HBM),
            pl.BlockSpec(memory_space=vmem),
        ],
        out_specs=[pl.BlockSpec(memory_space=vmem)] * 2,
        scratch_shapes=scratch,
        compiler_params=pltpu.CompilerParams(
            collective_id=0, has_side_effects=True, vmem_limit_bytes=46 * 2**20
        ),
        name="climate",
    )(field, counts)


STRIP = HOURS * TILES
WIDE = HOURS * 4 * SLOT
PAIRS = YEARS * DAYS // 2
GROUP = 2


def subtract_kernel(count_ref, field, climate, out, moved_on, ready, store_sem):
    size = GROUP * 2 * STRIP
    groups = PAIRS // GROUP

    @pl.loop(0, ROWS)
    def _(e):
        base = pl.multiple_of(e * (WIDE + 8), 8)
        value = climate[pl.ds(pl.multiple_of(e * WIDE, 8), STRIP), :]
        moved_on[pl.ds(base + 4, STRIP), :] = value

    sublane = lax.broadcasted_iota(jnp.int32, (8, LANES), 0)

    def row_of(k):
        y, s = divmod(k, DAYS)
        ahead = (count_ref[y, 0, s] < 0).astype(jnp.int32)
        return s + ahead

    stores = []
    body = STRIP - STRIP % 8
    for g in range(groups):
        for pair in range(g * GROUP, (g + 1) * GROUP):
            start = pair * 2 * STRIP
            even = pl.multiple_of(row_of(2 * pair) * WIDE, 8)
            odd = pl.multiple_of(row_of(2 * pair + 1) * (WIDE + 8), 8)

            def put(offset, size, value):
                span = pl.ds(start + offset, size)
                ready[span, :] = (field[span, :].astype(jnp.float32) - value).astype(jnp.bfloat16)

            put(0, body, climate[pl.ds(even, body), :])
            middle = jnp.where(
                sublane < 4, climate[pl.ds(even + body, 8), :], moved_on[pl.ds(odd, 8), :]
            )
            put(body, 8, middle)
            put(body + 8, body, moved_on[pl.ds(odd + 8, body), :])
        store = pltpu.make_async_copy(
            ready.at[pl.ds(g * size, size)], out.at[pl.ds(g * size, size)], store_sem.at[g]
        )
        store.start()
        stores.append(store)
    for store in stores:
        store.wait()


def anomaly_of(field, counts, climate):
    rows = YEARS * DAYS * STRIP
    groups = PAIRS // GROUP
    return pl.pallas_call(
        subtract_kernel,
        out_shape=jax.ShapeDtypeStruct((rows, LANES), jnp.bfloat16),
        in_specs=[
            pl.BlockSpec(memory_space=pltpu.SMEM),
            pl.BlockSpec(memory_space=pltpu.VMEM),
            pl.BlockSpec(memory_space=pltpu.VMEM),
        ],
        out_specs=pl.BlockSpec(memory_space=pltpu.HBM),
        scratch_shapes=[
            pltpu.VMEM((ROWS * (WIDE + 8), LANES), jnp.float32),
            pltpu.VMEM((rows, LANES), jnp.bfloat16),
            pltpu.SemaphoreType.DMA((groups,)),
        ],
        compiler_params=pltpu.CompilerParams(vmem_limit_bytes=40 * 2**20),
        name="anomaly",
    )(counts, field, climate)


def tile_rows(array):
    *lead, hours, cells = array.shape
    tiles = cells // LANES
    split = array.reshape(-1, hours, tiles, LANES)
    split = with_layout_constraint(split, Layout(major_to_minor=(0, 2, 1, 3)))
    return split.transpose(0, 2, 1, 3).reshape(-1, LANES)


def from_tile_rows(rows, shape):
    *lead, hours, cells = shape
    tiles = cells // LANES
    split = rows.reshape(-1, tiles, hours, LANES).transpose(0, 2, 1, 3)
    split = with_layout_constraint(split, Layout(major_to_minor=(0, 2, 1, 3)))
    return split.reshape(shape)


def local(field, day_index, sample_count):
    slot = lax.broadcasted_iota(jnp.int32, day_index.shape, 1) + lax.axis_index("day") * DAYS
    moved = (day_index != slot)[:, None, :]
    counts = jnp.transpose(sample_count, (0, 2, 1))
    counts = jnp.where(moved, -counts, counts)
    climate, field = climate_of(field, counts)
    anomaly = anomaly_of(tile_rows(field), counts, tile_rows(climate))
    anomaly = from_tile_rows(anomaly, field.shape)
    cells = TILES * LANES // lax.axis_size("year")
    share = lax.dynamic_slice(
        climate, (0, 0, lax.axis_index("year") * cells), (DAYS, HOURS, cells)
    )
    return anomaly, share.astype(jnp.bfloat16)


def solution(mesh):
    return jax.shard_map(
        local,
        mesh=mesh,
        in_specs=(P("year", "day", None, None), P("year", "day"), P("year", "day", None)),
        out_specs=(P("year", "day", None, None), P("day", None, "year")),
        check_vma=False,
    )
```

```python
import functools

import jax
import jax.numpy as jnp
from jax import lax
from jax.experimental import pallas as pl
from jax.experimental.layout import Layout, with_layout_constraint
from jax.experimental.pallas import tpu as pltpu
from jax.sharding import PartitionSpec as P

MESH = pl.DeviceIdType.MESH
HALF = 30
YEARS, DAYS, HOURS, TILES = 4, 23, 2, 90
LANES = 128
ROWS = DAYS + 1
MID = ROWS // 2
SLOT = 23
GROUPS = ((7, 6), (6, 4))
EDGE = ROWS // 3
MESSAGES = 8 + 44 * len(GROUPS)


def lanes(start, tiles):
    if isinstance(start, int):
        return pl.ds(start * LANES, tiles * LANES)
    return pl.ds(pl.multiple_of(start * LANES, LANES), tiles * LANES)


def rows_of(low):
    return pl.ds(0, MID) if low else pl.ds(MID, MID)


def shares(group):
    first, second = group
    return (first + 1) // 2, first // 2, second // 2


def reduce_kernel(
    field, count_ref, cl, held, part, weight, first_count, second_count,
    count0, count1, count2, count_x, count_z, count_d, kept, inverse, load_sem, send_sem, recv_sem,
    *buffers,
):
    day = lax.axis_index("day")
    year = lax.axis_index("year")
    days = lax.axis_size("day")
    z, u = year // 2, year % 2
    up, down, across = (z + 1) % 4, (z + 3) % 4, (z + 2) % 4
    at_up, at_down, at_across = (day, up * 2 + u), (day, down * 2 + u), (day, across * 2 + u)
    twin = (day, z * 2 + (1 - u))
    beside = [((day + step + days) % days, year) for step in (1, -1, 2, -2)]
    peers = [at_up, at_down, at_across, twin] + beside

    barrier = pltpu.get_barrier_semaphore()
    for peer in peers:
        pl.semaphore_signal(barrier, inc=1, device_id=peer, device_id_type=MESH)

    order = (across, up, down, z)
    inner = SLOT - 4 * SLOT + TILES
    loads = []
    for number, s in enumerate(order):
        span = lanes(s * SLOT, inner)
        loads.append((field.at[:, :, :, span], held.at[:, :, :, span], load_sem.at[number]))
    for s in range(3):
        span = lanes(s * SLOT + inner, SLOT - inner)
        loads.append((field.at[:, :, :, span], held.at[:, :, :, span], load_sem.at[4 + s]))
    loads = [pltpu.make_async_copy(*load) for load in loads]
    for load in loads[:1] + loads[4:] + loads[1:4]:
        load.start()

    used = []

    def copy(source, target, device):
        number = len(used)
        used.append(
            pltpu.make_async_remote_copy(
                src_ref=source, dst_ref=target, send_sem=send_sem.at[number],
                recv_sem=recv_sem.at[number], device_id=device, device_id_type=MESH,
            )
        )
        used[-1].start()
        return used[-1]

    total_own = jnp.zeros((HOURS, DAYS), jnp.float32)
    total_next = jnp.zeros((HOURS, DAYS), jnp.float32)
    for y in range(YEARS):
        counts = count_ref[y].astype(jnp.float32)
        own = jnp.maximum(counts, 0.0)
        after = jnp.maximum(-counts, 0.0)
        total_own += own
        total_next += after
        for s in range(DAYS):
            weight[y, s] = jnp.broadcast_to(own[:, s : s + 1], (HOURS, 4 * LANES))
            weight[y, DAYS + s] = jnp.broadcast_to(after[:, s : s + 1], (HOURS, 4 * LANES))
    first_count[...] = jnp.zeros_like(first_count)
    second_count[...] = jnp.zeros_like(second_count)
    first_count[:, :DAYS] = total_own
    second_count[:, :DAYS] = total_next
    count0[...] = first_count[...] + pltpu.roll(second_count[...], 1, 1)

    def add_years(start, tiles):
        halves = [(h, min(4, tiles - h)) for h in range(0, tiles, 4)]
        carried = [None] * len(halves)
        for s in range(DAYS):
            own = [None] * len(halves)
            after = [None] * len(halves)
            for y in range(YEARS):
                value = held[y, s, :, lanes(start, tiles)].astype(jnp.float32)
                for n, (h, width) in enumerate(halves):
                    piece = value[:, h * LANES : (h + width) * LANES]
                    a = piece * weight[y, s, :, : width * LANES]
                    b = piece * weight[y, DAYS + s, :, : width * LANES]
                    own[n] = a if y == 0 else own[n] + a
                    after[n] = b if y == 0 else after[n] + b
            for n, (h, width) in enumerate(halves):
                row = own[n] if s == 0 else own[n] + carried[n]
                part[s, :, lanes(start + h, width)] = row
            carried = after
        for n, (h, width) in enumerate(halves):
            part[DAYS, :, lanes(start + h, width)] = carried[n]

    part[:, :, TILES * LANES :] = jnp.zeros((ROWS, HOURS, (4 * SLOT - TILES) * LANES), jnp.float32)
    added = []

    def ready(number):
        while len(added) <= number:
            s = order[len(added)]
            for load in loads[:1] + loads[4:] if not added else loads[len(added) : len(added) + 1]:
                load.wait()
            start = s * SLOT

            @pl.loop(0, inner // 8)
            def _(step):
                add_years(start + step * 8, 8)

            add_years(start + inner // 8 * 8, inner % 8)

            @pl.when(s < 3)
            def _():
                add_years(start + inner, SLOT - inner)

            added.append(s)

    ready(0)
    pl.semaphore_wait(barrier, len(peers))

    class Ring:
        def __init__(self, buffers, at, tiles):
            self.buffers, self.at, self.tiles = buffers, at, tiles

        def piece(self, low, s):
            return part.at[rows_of(low), :, lanes(self.at(s), self.tiles)]

        def begin(self):
            ready(0)
            self.far_up = copy(self.piece(True, across), self.buffers.at[0], at_up)
            self.far_down = copy(self.piece(False, across), self.buffers.at[1], at_down)

        def near_up(self):
            ready(1)
            self.up = copy(self.piece(False, up), self.buffers.at[2], at_up)

        def near_down(self):
            ready(2)
            self.down = copy(self.piece(True, down), self.buffers.at[3], at_down)

        def forward(self):
            ready(2)
            self.far_up.wait_recv()
            self.add(True, up, 0)
            self.on_up = copy(self.piece(True, up), self.buffers.at[4], at_up)
            self.far_down.wait_recv()
            self.add(False, down, 1)
            self.on_down = copy(self.piece(False, down), self.buffers.at[5], at_down)

        def add(self, low, s, number):
            where = (rows_of(low), slice(None), lanes(self.at(s), self.tiles))
            part[where] = part[where] + self.buffers[number]

        def result(self):
            ready(3)
            self.up.wait_recv()
            self.down.wait_recv()
            self.on_up.wait_recv()
            self.on_down.wait_recv()
            where = lanes(self.at(z), self.tiles)
            low = part[rows_of(True), :, where] + self.buffers[3] + self.buffers[4]
            high = part[rows_of(False), :, where] + self.buffers[2] + self.buffers[5]
            return low, high

    class Spread:
        def __init__(self, at, tiles):
            self.at, self.tiles = at, tiles

        def send(self, low, s, device):
            piece = cl.at[rows_of(low), :, lanes(self.at(s), self.tiles)]
            return copy(piece, piece, device)

        def begin(self):
            self.up0 = self.send(True, z, at_up)
            self.down0 = self.send(False, z, at_down)
            self.up1 = self.send(False, z, at_up)
            self.down1 = self.send(True, z, at_down)

        def forward(self):
            self.up0.wait_recv()
            self.up2 = self.send(True, down, at_up)
            self.down0.wait_recv()
            self.down2 = self.send(False, up, at_down)

        def near(self):
            self.up1.wait_recv()
            self.down1.wait_recv()

        def far(self):
            self.up2.wait_recv()
            self.down2.wait_recv()

    class Group:
        def __init__(self, number):
            self.first, self.second = GROUPS[number]
            start = sum(map(sum, GROUPS[:number]))
            self.share, self.stride, self.half = shares(GROUPS[number])
            first_in, second_in, self.second_x, self.first_x, self.own, self.window = buffers[
                6 * number : 6 * number + 6
            ]
            self.first_at = lambda s: s * SLOT + start
            self.second_at = lambda s: s * SLOT + start + self.first
            self.kept_at = lambda s: self.second_at(s) + u * self.half
            self.ring = Ring(first_in, self.first_at, self.first)
            self.late_ring = Ring(second_in, self.kept_at, self.half)
            self.own_spread = Spread(lambda s: self.first_at(s) + u * self.stride, self.share)
            self.other_spread = Spread(
                lambda s: self.first_at(s) + (1 - u) * self.share, self.stride
            )
            self.late_spread = Spread(self.kept_at, self.half)
            self.swaps = []
            self.last = []

        def swap(self, *numbers):
            for number in numbers:
                ready(number)
                start = self.second_at(order[number]) + (1 - u) * self.half
                source = part.at[:, :, lanes(start, self.half)]
                self.swaps.append(copy(source, self.second_x.at[number], twin))

        def swapped(self, number):
            self.swaps[number].wait_recv()
            where = (slice(None), slice(None), lanes(self.kept_at(order[number]), self.half))
            part[where] = part[where] + self.second_x[number]

        def near(self):
            self.ring.near_up()
            self.ring.near_down()

        def late_begin(self):
            self.swapped(0)
            self.late_ring.begin()

        def late_near(self):
            self.swapped(1)
            self.late_ring.near_up()
            self.swapped(2)
            self.late_ring.near_down()

        def swap_first(self):
            low, high = self.ring.result()
            where = lanes(self.first_at(z), self.first)
            part[rows_of(True), :, where] = low
            part[rows_of(False), :, where] = high
            start = self.first_at(z) + (1 - u) * self.stride
            self.pair = copy(part.at[:, :, lanes(start, self.share)], self.first_x, twin)

        def late_result(self):
            self.swapped(3)
            low, high = self.late_ring.result()
            span = pl.ds(self.share * LANES, self.half * LANES)
            self.own[rows_of(True), :, span] = low
            self.own[rows_of(False), :, span] = high

        def share_out(self):
            self.pair.wait_recv()
            span = lanes(self.first_at(z) + u * self.stride, self.share)
            self.own[:, :, : self.share * LANES] = part[:, :, span] + self.first_x[...]
            right, left, right2, left2 = beside
            own, window = self.own, self.window
            self.out = [
                copy(own, window.at[pl.ds(0, ROWS)], right),
                copy(own, window.at[pl.ds(ROWS, ROWS)], left),
                copy(own.at[pl.ds(ROWS - EDGE, EDGE)], window.at[pl.ds(2 * ROWS, EDGE)], right2),
                copy(own.at[pl.ds(0, EDGE)], window.at[pl.ds(2 * ROWS + EDGE, EDGE)], left2),
            ]

        def smooth(self):
            for message in self.out:
                message.wait_recv()
            own, window = self.own, self.window

            def day_row(offset, span):
                if offset < -DAYS:
                    return window[2 * ROWS + offset + 2 * DAYS - (ROWS - EDGE), :, span]
                if offset == -DAYS:
                    return window[0, :, span] + window[2 * ROWS + EDGE - 1, :, span]
                if offset < 0:
                    return window[offset + DAYS, :, span]
                if offset == 0:
                    return own[0, :, span] + window[DAYS, :, span]
                if offset < DAYS:
                    return own[offset, :, span]
                if offset == DAYS:
                    return window[ROWS, :, span] + own[DAYS, :, span]
                if offset < 2 * DAYS:
                    return window[ROWS + offset - DAYS, :, span]
                if offset == 2 * DAYS:
                    return window[2 * ROWS + EDGE, :, span] + window[ROWS + DAYS, :, span]
                return window[2 * ROWS + EDGE + offset - 2 * DAYS, :, span]

            def smoothed(start, at, tiles):
                for h in range(0, tiles, 4):
                    width = min(4, tiles - h)
                    span = pl.ds((start + h) * LANES, width * LANES)
                    total = day_row(0, span)
                    for offset in range(1, DAYS):
                        total = total + day_row(offset, span)
                    for offset in range(-1, -HALF - 1, -1):
                        total = total + day_row(offset, span)
                        if offset + HALF < ROWS:
                            kept[offset + HALF, :, : width * LANES] = total
                    total = None
                    for offset in range(DAYS, DAYS + HALF + 1):
                        row = day_row(offset, span)
                        total = row if total is None else total + row
                        if offset >= HALF:
                            i = offset - HALF
                            sums = kept[i, :, : width * LANES] + total
                            scaled = sums * inverse[i, :, : width * LANES]
                            cl[i, :, lanes(at + h, width)] = scaled

            smoothed(0, self.first_at(z) + u * self.stride, self.share)
            smoothed(self.share, self.kept_at(z), self.half)

        def across_x(self, s):
            piece = cl.at[:, :, lanes(self.kept_at(s), self.half)]
            self.last.append(copy(piece, piece, twin))

        def spread_second(self):
            self.late_spread.begin()
            self.across_x(z)

        def spread_first(self):
            piece = cl.at[:, :, lanes(self.first_at(z) + u * self.share, self.stride)]
            self.pair = copy(piece, piece, twin)
            self.own_spread.begin()

        def late_forward(self):
            self.late_spread.forward()

        def late_across(self):
            self.late_spread.near()
            self.across_x(up)
            self.across_x(down)

        def other(self):
            self.pair.wait_recv()
            self.other_spread.begin()

        def late_far(self):
            self.late_spread.far()
            self.across_x(across)

        def end(self):
            for portion in (self.own_spread, self.other_spread):
                portion.near()
                portion.far()
            for message in self.last:
                message.wait_recv()

    def windows():
        for message in aside:
            message.wait_recv()
        spread = (
            count_d[2]
            + pltpu.roll(count_d[0], DAYS, 1)
            + pltpu.roll(count2[...], 2 * DAYS, 1)
            + pltpu.roll(count_d[1], 3 * DAYS, 1)
            + pltpu.roll(count_d[3], 4 * DAYS, 1)
        )
        lane = lax.broadcasted_iota(jnp.int32, (HOURS, LANES), 1)
        for i in range(ROWS):
            start = 2 * DAYS - HALF + i
            inside = (lane >= start) & (lane <= start + 2 * HALF)
            count = jnp.sum(jnp.where(inside, spread, 0.0), axis=1, keepdims=True)
            inverse[i] = jnp.broadcast_to(1.0 / count, (HOURS, 4 * LANES))

    send_count = copy(count0, count_x, twin)
    one, two = (Group(number) for number in range(len(GROUPS)))
    one.ring.begin()
    two.swap(0)
    one.swap(0)
    two.swap(1)
    one.swap(1, 2)
    two.ring.begin()
    two.swap(2)
    one.near()
    send_count.wait_recv()
    count1[...] = count0[...] + count_x[...]
    along = [copy(count1, count_z.at[n], d) for n, d in enumerate((at_up, at_down, at_across))]
    one.ring.forward()
    one.late_begin()
    two.ring.forward()
    one.swap(3)
    two.near()
    one.swap_first()
    one.late_near()
    two.swap(3)
    one.late_ring.forward()
    two.late_begin()
    two.swap_first()
    one.late_result()
    two.late_near()
    for message in along:
        message.wait_recv()
    count2[...] = count1[...] + count_z[0] + count_z[1] + count_z[2]
    aside = [copy(count2, count_d.at[n], d) for n, d in enumerate(beside)]
    one.share_out()
    two.late_ring.forward()
    two.late_result()
    two.share_out()
    windows()
    one.smooth()
    one.spread_second()
    one.spread_first()
    two.smooth()
    two.spread_second()
    one.late_forward()
    two.spread_first()
    one.late_across()
    two.late_forward()
    two.late_across()
    one.other()
    one.late_far()
    two.own_spread.forward()
    two.other()
    two.late_far()
    one.own_spread.forward()
    one.other_spread.forward()
    two.other_spread.forward()
    for group in (one, two):
        group.end()
    for message in used:
        message.wait_send()


def climate_of(field, counts):
    f32 = jnp.float32
    wide = 4 * SLOT * LANES
    vmem = pltpu.VMEM
    row = (HOURS, LANES)
    scratch = [
        vmem((ROWS, HOURS, wide), f32),
        vmem((YEARS, 2 * DAYS, HOURS, 4 * LANES), f32),
        vmem(row, f32), vmem(row, f32), vmem(row, f32), vmem(row, f32), vmem(row, f32),
        vmem(row, f32), vmem((3, *row), f32), vmem((4, *row), f32),
        vmem((ROWS, HOURS, 4 * LANES), f32),
        vmem((ROWS, HOURS, 4 * LANES), f32),
        pltpu.SemaphoreType.DMA((7,)),
        pltpu.SemaphoreType.DMA((MESSAGES,)),
        pltpu.SemaphoreType.DMA((MESSAGES,)),
    ]
    for group in GROUPS:
        share, _, half = shares(group)
        together = (share + half) * LANES
        scratch += [
            vmem((6, MID, HOURS, group[0] * LANES), f32),
            vmem((6, MID, HOURS, half * LANES), f32),
            vmem((4, ROWS, HOURS, half * LANES), f32),
            vmem((ROWS, HOURS, share * LANES), f32),
            vmem((ROWS, HOURS, together), f32),
            vmem((2 * ROWS + 2 * EDGE, HOURS, together), f32),
        ]
    return pl.pallas_call(
        reduce_kernel,
        out_shape=(
            jax.ShapeDtypeStruct((ROWS, HOURS, wide), f32),
            jax.ShapeDtypeStruct(field.shape, field.dtype),
        ),
        in_specs=[
            pl.BlockSpec(memory_space=pltpu.HBM),
            pl.BlockSpec(memory_space=vmem),
        ],
        out_specs=[pl.BlockSpec(memory_space=vmem)] * 2,
        scratch_shapes=scratch,
        compiler_params=pltpu.CompilerParams(
            collective_id=0, has_side_effects=True, vmem_limit_bytes=46 * 2**20
        ),
        name="climate",
    )(field, counts)


STRIP = HOURS * TILES
WIDE = HOURS * 4 * SLOT
PAIRS = YEARS * DAYS // 2
GROUP = 2


def subtract_kernel(count_ref, field, climate, out, moved_on, ready, store_sem):
    size = GROUP * 2 * STRIP
    groups = PAIRS // GROUP

    @pl.loop(0, ROWS)
    def _(e):
        base = pl.multiple_of(e * (WIDE + 8), 8)
        value = climate[pl.ds(pl.multiple_of(e * WIDE, 8), STRIP), :]
        moved_on[pl.ds(base + 4, STRIP), :] = value

    sublane = lax.broadcasted_iota(jnp.int32, (8, LANES), 0)

    def row_of(k):
        y, s = divmod(k, DAYS)
        ahead = (count_ref[y, 0, s] < 0).astype(jnp.int32)
        return s + ahead

    stores = []
    body = STRIP - STRIP % 8
    for g in range(groups):
        for pair in range(g * GROUP, (g + 1) * GROUP):
            start = pair * 2 * STRIP
            even = pl.multiple_of(row_of(2 * pair) * WIDE, 8)
            odd = pl.multiple_of(row_of(2 * pair + 1) * (WIDE + 8), 8)

            def put(offset, size, value):
                span = pl.ds(start + offset, size)
                ready[span, :] = (field[span, :].astype(jnp.float32) - value).astype(jnp.bfloat16)

            put(0, body, climate[pl.ds(even, body), :])
            middle = jnp.where(
                sublane < 4, climate[pl.ds(even + body, 8), :], moved_on[pl.ds(odd, 8), :]
            )
            put(body, 8, middle)
            put(body + 8, body, moved_on[pl.ds(odd + 8, body), :])
        store = pltpu.make_async_copy(
            ready.at[pl.ds(g * size, size)], out.at[pl.ds(g * size, size)], store_sem.at[g]
        )
        store.start()
        stores.append(store)
    for store in stores:
        store.wait()


def anomaly_of(field, counts, climate):
    rows = YEARS * DAYS * STRIP
    groups = PAIRS // GROUP
    return pl.pallas_call(
        subtract_kernel,
        out_shape=jax.ShapeDtypeStruct((rows, LANES), jnp.bfloat16),
        in_specs=[
            pl.BlockSpec(memory_space=pltpu.SMEM),
            pl.BlockSpec(memory_space=pltpu.VMEM),
            pl.BlockSpec(memory_space=pltpu.VMEM),
        ],
        out_specs=pl.BlockSpec(memory_space=pltpu.HBM),
        scratch_shapes=[
            pltpu.VMEM((ROWS * (WIDE + 8), LANES), jnp.float32),
            pltpu.VMEM((rows, LANES), jnp.bfloat16),
            pltpu.SemaphoreType.DMA((groups,)),
        ],
        compiler_params=pltpu.CompilerParams(vmem_limit_bytes=40 * 2**20),
        name="anomaly",
    )(counts, field, climate)


def tile_rows(array):
    *lead, hours, cells = array.shape
    tiles = cells // LANES
    split = array.reshape(-1, hours, tiles, LANES)
    split = with_layout_constraint(split, Layout(major_to_minor=(0, 2, 1, 3)))
    return split.transpose(0, 2, 1, 3).reshape(-1, LANES)


def from_tile_rows(rows, shape):
    *lead, hours, cells = shape
    tiles = cells // LANES
    split = rows.reshape(-1, tiles, hours, LANES).transpose(0, 2, 1, 3)
    split = with_layout_constraint(split, Layout(major_to_minor=(0, 2, 1, 3)))
    return split.reshape(shape)


def local(field, day_index, sample_count):
    slot = lax.broadcasted_iota(jnp.int32, sample_count.shape, 1) + lax.axis_index("day") * DAYS
    counts = jnp.where(day_index[:, :, None] != slot, -sample_count, sample_count)
    counts = jnp.transpose(counts, (0, 2, 1))
    climate, field = climate_of(field, counts)
    anomaly = anomaly_of(tile_rows(field), counts, tile_rows(climate))
    anomaly = from_tile_rows(anomaly, field.shape)
    cells = TILES * LANES // lax.axis_size("year")
    share = lax.dynamic_slice(
        climate, (0, 0, lax.axis_index("year") * cells), (DAYS, HOURS, cells)
    )
    return anomaly, share.astype(jnp.bfloat16)


def solution(mesh):
    return jax.shard_map(
        local,
        mesh=mesh,
        in_specs=(P("year", "day", None, None), P("year", "day"), P("year", "day", None)),
        out_specs=(P("year", "day", None, None), P("day", None, "year")),
        check_vma=False,
    )
```

```python
import functools

import jax
import jax.numpy as jnp
from jax import lax
from jax.experimental import pallas as pl
from jax.experimental.layout import Layout, with_layout_constraint
from jax.experimental.pallas import tpu as pltpu
from jax.sharding import PartitionSpec as P

MESH = pl.DeviceIdType.MESH
HALF = 30
YEARS, DAYS, HOURS, TILES = 4, 23, 2, 90
LANES = 128
ROWS = DAYS + 1
MID = ROWS // 2
SLOT = 23
GROUPS = ((7, 6), (6, 4))
EDGE = ROWS // 3
MESSAGES = 8 + 44 * len(GROUPS)


def lanes(start, tiles):
    if isinstance(start, int):
        return pl.ds(start * LANES, tiles * LANES)
    return pl.ds(pl.multiple_of(start * LANES, LANES), tiles * LANES)


def rows_of(low):
    return pl.ds(0, MID) if low else pl.ds(MID, MID)


def shares(group):
    first, second = group
    return (first + 1) // 2, first // 2, second // 2


def reduce_kernel(
    field, count_ref, cl, held, part, weight, first_count, second_count,
    count0, count1, count2, count_x, count_z, count_d, kept, inverse, load_sem, send_sem, recv_sem,
    *buffers,
):
    day = lax.axis_index("day")
    year = lax.axis_index("year")
    days = lax.axis_size("day")
    z, u = year // 2, year % 2
    up, down, across = (z + 1) % 4, (z + 3) % 4, (z + 2) % 4
    at_up, at_down, at_across = (day, up * 2 + u), (day, down * 2 + u), (day, across * 2 + u)
    twin = (day, z * 2 + (1 - u))
    beside = [((day + step + days) % days, year) for step in (1, -1, 2, -2)]
    peers = [at_up, at_down, at_across, twin] + beside

    barrier = pltpu.get_barrier_semaphore()
    for peer in peers:
        pl.semaphore_signal(barrier, inc=1, device_id=peer, device_id_type=MESH)

    order = (across, up, down, z)
    inner = SLOT - 4 * SLOT + TILES
    loads = []
    for number, s in enumerate(order):
        span = lanes(s * SLOT, inner)
        loads.append((field.at[:, :, :, span], held.at[:, :, :, span], load_sem.at[number]))
    for s in range(3):
        span = lanes(s * SLOT + inner, SLOT - inner)
        loads.append((field.at[:, :, :, span], held.at[:, :, :, span], load_sem.at[4 + s]))
    loads = [pltpu.make_async_copy(*load) for load in loads]
    for load in loads[:1] + loads[4:] + loads[1:4]:
        load.start()

    used = []

    def copy(source, target, device):
        number = len(used)
        used.append(
            pltpu.make_async_remote_copy(
                src_ref=source, dst_ref=target, send_sem=send_sem.at[number],
                recv_sem=recv_sem.at[number], device_id=device, device_id_type=MESH,
            )
        )
        used[-1].start()
        return used[-1]

    total_own = jnp.zeros((HOURS, DAYS), jnp.float32)
    total_next = jnp.zeros((HOURS, DAYS), jnp.float32)
    for y in range(YEARS):
        counts = count_ref[y].astype(jnp.float32)
        own = jnp.maximum(counts, 0.0)
        after = jnp.maximum(-counts, 0.0)
        total_own += own
        total_next += after
        for s in range(DAYS):
            weight[y, s] = jnp.broadcast_to(own[:, s : s + 1], (HOURS, 4 * LANES))
            weight[y, DAYS + s] = jnp.broadcast_to(after[:, s : s + 1], (HOURS, 4 * LANES))
    first_count[...] = jnp.zeros_like(first_count)
    second_count[...] = jnp.zeros_like(second_count)
    first_count[:, :DAYS] = total_own
    second_count[:, :DAYS] = total_next
    count0[...] = first_count[...] + pltpu.roll(second_count[...], 1, 1)

    def add_years(start, tiles):
        halves = [(h, min(4, tiles - h)) for h in range(0, tiles, 4)]
        carried = [None] * len(halves)
        for s in range(DAYS):
            own = [None] * len(halves)
            after = [None] * len(halves)
            for y in range(YEARS):
                value = held[y, s, :, lanes(start, tiles)].astype(jnp.float32)
                for n, (h, width) in enumerate(halves):
                    piece = value[:, h * LANES : (h + width) * LANES]
                    a = piece * weight[y, s, :, : width * LANES]
                    b = piece * weight[y, DAYS + s, :, : width * LANES]
                    own[n] = a if y == 0 else own[n] + a
                    after[n] = b if y == 0 else after[n] + b
            for n, (h, width) in enumerate(halves):
                row = own[n] if s == 0 else own[n] + carried[n]
                part[s, :, lanes(start + h, width)] = row
            carried = after
        for n, (h, width) in enumerate(halves):
            part[DAYS, :, lanes(start + h, width)] = carried[n]

    part[:, :, TILES * LANES :] = jnp.zeros((ROWS, HOURS, (4 * SLOT - TILES) * LANES), jnp.float32)
    added = []

    def ready(number):
        while len(added) <= number:
            s = order[len(added)]
            for load in loads[:1] + loads[4:] if not added else loads[len(added) : len(added) + 1]:
                load.wait()
            start = s * SLOT

            @pl.loop(0, inner // 8)
            def _(step):
                add_years(start + step * 8, 8)

            add_years(start + inner // 8 * 8, inner % 8)

            @pl.when(s < 3)
            def _():
                add_years(start + inner, SLOT - inner)

            added.append(s)

    ready(0)
    pl.semaphore_wait(barrier, len(peers))

    class Ring:
        def __init__(self, buffers, at, tiles):
            self.buffers, self.at, self.tiles = buffers, at, tiles

        def piece(self, low, s):
            return part.at[rows_of(low), :, lanes(self.at(s), self.tiles)]

        def begin(self):
            ready(0)
            self.far_up = copy(self.piece(True, across), self.buffers.at[0], at_up)
            self.far_down = copy(self.piece(False, across), self.buffers.at[1], at_down)

        def near_up(self):
            ready(1)
            self.up = copy(self.piece(False, up), self.buffers.at[2], at_up)

        def near_down(self):
            ready(2)
            self.down = copy(self.piece(True, down), self.buffers.at[3], at_down)

        def forward(self):
            ready(2)
            self.far_up.wait_recv()
            self.add(True, up, 0)
            self.on_up = copy(self.piece(True, up), self.buffers.at[4], at_up)
            self.far_down.wait_recv()
            self.add(False, down, 1)
            self.on_down = copy(self.piece(False, down), self.buffers.at[5], at_down)

        def add(self, low, s, number):
            where = (rows_of(low), slice(None), lanes(self.at(s), self.tiles))
            part[where] = part[where] + self.buffers[number]

        def result(self):
            ready(3)
            self.up.wait_recv()
            self.down.wait_recv()
            self.on_up.wait_recv()
            self.on_down.wait_recv()
            where = lanes(self.at(z), self.tiles)
            low = part[rows_of(True), :, where] + self.buffers[3] + self.buffers[4]
            high = part[rows_of(False), :, where] + self.buffers[2] + self.buffers[5]
            return low, high

    class Spread:
        def __init__(self, at, tiles):
            self.at, self.tiles = at, tiles

        def send(self, low, s, device):
            piece = cl.at[rows_of(low), :, lanes(self.at(s), self.tiles)]
            return copy(piece, piece, device)

        def begin(self):
            self.up0 = self.send(True, z, at_up)
            self.down0 = self.send(False, z, at_down)
            self.up1 = self.send(False, z, at_up)
            self.down1 = self.send(True, z, at_down)

        def forward(self):
            self.up0.wait_recv()
            self.up2 = self.send(True, down, at_up)
            self.down0.wait_recv()
            self.down2 = self.send(False, up, at_down)

        def near(self):
            self.up1.wait_recv()
            self.down1.wait_recv()

        def far(self):
            self.up2.wait_recv()
            self.down2.wait_recv()

    class Group:
        def __init__(self, number):
            self.first, self.second = GROUPS[number]
            start = sum(map(sum, GROUPS[:number]))
            self.share, self.stride, self.half = shares(GROUPS[number])
            first_in, second_in, self.second_x, self.first_x, self.own, self.window = buffers[
                6 * number : 6 * number + 6
            ]
            self.first_at = lambda s: s * SLOT + start
            self.second_at = lambda s: s * SLOT + start + self.first
            self.kept_at = lambda s: self.second_at(s) + u * self.half
            self.ring = Ring(first_in, self.first_at, self.first)
            self.late_ring = Ring(second_in, self.kept_at, self.half)
            self.own_spread = Spread(lambda s: self.first_at(s) + u * self.stride, self.share)
            self.other_spread = Spread(
                lambda s: self.first_at(s) + (1 - u) * self.share, self.stride
            )
            self.late_spread = Spread(self.kept_at, self.half)
            self.swaps = []
            self.last = []

        def swap(self, *numbers):
            for number in numbers:
                ready(number)
                start = self.second_at(order[number]) + (1 - u) * self.half
                source = part.at[:, :, lanes(start, self.half)]
                self.swaps.append(copy(source, self.second_x.at[number], twin))

        def swapped(self, number):
            self.swaps[number].wait_recv()
            where = (slice(None), slice(None), lanes(self.kept_at(order[number]), self.half))
            part[where] = part[where] + self.second_x[number]

        def near(self):
            self.ring.near_up()
            self.ring.near_down()

        def late_begin(self):
            self.swapped(0)
            self.late_ring.begin()

        def late_near(self):
            self.swapped(1)
            self.late_ring.near_up()
            self.swapped(2)
            self.late_ring.near_down()

        def swap_first(self):
            low, high = self.ring.result()
            where = lanes(self.first_at(z), self.first)
            part[rows_of(True), :, where] = low
            part[rows_of(False), :, where] = high
            start = self.first_at(z) + (1 - u) * self.stride
            self.pair = copy(part.at[:, :, lanes(start, self.share)], self.first_x, twin)

        def late_result(self):
            self.swapped(3)
            low, high = self.late_ring.result()
            span = pl.ds(self.share * LANES, self.half * LANES)
            self.own[rows_of(True), :, span] = low
            self.own[rows_of(False), :, span] = high

        def share_out(self):
            self.pair.wait_recv()
            span = lanes(self.first_at(z) + u * self.stride, self.share)
            self.own[:, :, : self.share * LANES] = part[:, :, span] + self.first_x[...]
            right, left, right2, left2 = beside
            own, window = self.own, self.window
            self.out = [
                copy(own, window.at[pl.ds(0, ROWS)], right),
                copy(own, window.at[pl.ds(ROWS, ROWS)], left),
                copy(own.at[pl.ds(ROWS - EDGE, EDGE)], window.at[pl.ds(2 * ROWS, EDGE)], right2),
                copy(own.at[pl.ds(0, EDGE)], window.at[pl.ds(2 * ROWS + EDGE, EDGE)], left2),
            ]

        def smooth(self):
            for message in self.out:
                message.wait_recv()
            own, window = self.own, self.window

            def day_row(offset, span):
                if offset < -DAYS:
                    return window[2 * ROWS + offset + 2 * DAYS - (ROWS - EDGE), :, span]
                if offset == -DAYS:
                    return window[0, :, span] + window[2 * ROWS + EDGE - 1, :, span]
                if offset < 0:
                    return window[offset + DAYS, :, span]
                if offset == 0:
                    return own[0, :, span] + window[DAYS, :, span]
                if offset < DAYS:
                    return own[offset, :, span]
                if offset == DAYS:
                    return window[ROWS, :, span] + own[DAYS, :, span]
                if offset < 2 * DAYS:
                    return window[ROWS + offset - DAYS, :, span]
                if offset == 2 * DAYS:
                    return window[2 * ROWS + EDGE, :, span] + window[ROWS + DAYS, :, span]
                return window[2 * ROWS + EDGE + offset - 2 * DAYS, :, span]

            def smoothed(start, at, tiles):
                for h in range(0, tiles, 4):
                    width = min(4, tiles - h)
                    span = pl.ds((start + h) * LANES, width * LANES)
                    total = day_row(0, span)
                    for offset in range(1, DAYS):
                        total = total + day_row(offset, span)
                    for offset in range(-1, -HALF - 1, -1):
                        total = total + day_row(offset, span)
                        if offset + HALF < ROWS:
                            kept[offset + HALF, :, : width * LANES] = total
                    total = None
                    for offset in range(DAYS, DAYS + HALF + 1):
                        row = day_row(offset, span)
                        total = row if total is None else total + row
                        if offset >= HALF:
                            i = offset - HALF
                            sums = kept[i, :, : width * LANES] + total
                            scaled = sums * inverse[i, :, : width * LANES]
                            cl[i, :, lanes(at + h, width)] = scaled

            smoothed(0, self.first_at(z) + u * self.stride, self.share)
            smoothed(self.share, self.kept_at(z), self.half)

        def across_x(self, s):
            piece = cl.at[:, :, lanes(self.kept_at(s), self.half)]
            self.last.append(copy(piece, piece, twin))

        def spread_second(self):
            self.late_spread.begin()
            self.across_x(z)

        def spread_first(self):
            piece = cl.at[:, :, lanes(self.first_at(z) + u * self.share, self.stride)]
            self.pair = copy(piece, piece, twin)
            self.own_spread.begin()

        def late_forward(self):
            self.late_spread.forward()

        def late_across(self):
            self.late_spread.near()
            self.across_x(up)
            self.across_x(down)

        def other(self):
            self.pair.wait_recv()
            self.other_spread.begin()

        def late_far(self):
            self.late_spread.far()
            self.across_x(across)

        def end(self):
            for portion in (self.own_spread, self.other_spread):
                portion.near()
                portion.far()
            for message in self.last:
                message.wait_recv()

    def windows():
        for message in aside:
            message.wait_recv()
        spread = (
            count_d[2]
            + pltpu.roll(count_d[0], DAYS, 1)
            + pltpu.roll(count2[...], 2 * DAYS, 1)
            + pltpu.roll(count_d[1], 3 * DAYS, 1)
            + pltpu.roll(count_d[3], 4 * DAYS, 1)
        )
        lane = lax.broadcasted_iota(jnp.int32, (HOURS, LANES), 1)
        for i in range(ROWS):
            start = 2 * DAYS - HALF + i
            inside = (lane >= start) & (lane <= start + 2 * HALF)
            count = jnp.sum(jnp.where(inside, spread, 0.0), axis=1, keepdims=True)
            inverse[i] = jnp.broadcast_to(1.0 / count, (HOURS, 4 * LANES))

    send_count = copy(count0, count_x, twin)
    one, two = (Group(number) for number in range(len(GROUPS)))
    one.ring.begin()
    two.swap(0)
    one.swap(0)
    two.swap(1)
    one.swap(1, 2)
    two.ring.begin()
    two.swap(2)
    one.near()
    send_count.wait_recv()
    count1[...] = count0[...] + count_x[...]
    along = [copy(count1, count_z.at[n], d) for n, d in enumerate((at_up, at_down, at_across))]
    one.ring.forward()
    one.late_begin()
    two.ring.forward()
    one.swap(3)
    two.near()
    one.swap_first()
    one.late_near()
    two.swap(3)
    one.late_ring.forward()
    two.late_begin()
    two.swap_first()
    one.late_result()
    two.late_near()
    for message in along:
        message.wait_recv()
    count2[...] = count1[...] + count_z[0] + count_z[1] + count_z[2]
    aside = [copy(count2, count_d.at[n], d) for n, d in enumerate(beside)]
    one.share_out()
    two.late_ring.forward()
    two.late_result()
    two.share_out()
    windows()
    one.smooth()
    one.spread_second()
    one.spread_first()
    two.smooth()
    two.spread_second()
    one.late_forward()
    two.spread_first()
    one.late_across()
    two.late_forward()
    two.late_across()
    one.other()
    one.late_far()
    two.own_spread.forward()
    two.other()
    two.late_far()
    one.own_spread.forward()
    one.other_spread.forward()
    two.other_spread.forward()
    for group in (one, two):
        group.end()
    for message in used:
        message.wait_send()


def climate_of(field, counts):
    f32 = jnp.float32
    wide = 4 * SLOT * LANES
    vmem = pltpu.VMEM
    row = (HOURS, LANES)
    scratch = [
        vmem((ROWS, HOURS, wide), f32),
        vmem((YEARS, 2 * DAYS, HOURS, 4 * LANES), f32),
        vmem(row, f32), vmem(row, f32), vmem(row, f32), vmem(row, f32), vmem(row, f32),
        vmem(row, f32), vmem((3, *row), f32), vmem((4, *row), f32),
        vmem((ROWS, HOURS, 4 * LANES), f32),
        vmem((ROWS, HOURS, 4 * LANES), f32),
        pltpu.SemaphoreType.DMA((7,)),
        pltpu.SemaphoreType.DMA((MESSAGES,)),
        pltpu.SemaphoreType.DMA((MESSAGES,)),
    ]
    for group in GROUPS:
        share, _, half = shares(group)
        together = (share + half) * LANES
        scratch += [
            vmem((6, MID, HOURS, group[0] * LANES), f32),
            vmem((6, MID, HOURS, half * LANES), f32),
            vmem((4, ROWS, HOURS, half * LANES), f32),
            vmem((ROWS, HOURS, share * LANES), f32),
            vmem((ROWS, HOURS, together), f32),
            vmem((2 * ROWS + 2 * EDGE, HOURS, together), f32),
        ]
    return pl.pallas_call(
        reduce_kernel,
        out_shape=(
            jax.ShapeDtypeStruct((ROWS, HOURS, wide), f32),
            jax.ShapeDtypeStruct(field.shape, field.dtype),
        ),
        in_specs=[
            pl.BlockSpec(memory_space=pltpu.HBM),
            pl.BlockSpec(memory_space=vmem),
        ],
        out_specs=[pl.BlockSpec(memory_space=vmem)] * 2,
        scratch_shapes=scratch,
        compiler_params=pltpu.CompilerParams(
            collective_id=0, has_side_effects=True, vmem_limit_bytes=46 * 2**20
        ),
        name="climate",
    )(field, counts)


STRIP = HOURS * TILES
WIDE = HOURS * 4 * SLOT
PAIRS = YEARS * DAYS // 2
GROUP = 2


def subtract_kernel(count_ref, field, climate, by_hour, out, share, ready, cut, store_sem):
    size = GROUP * 2 * STRIP
    groups = PAIRS // GROUP
    sublane = lax.broadcasted_iota(jnp.int32, (8, LANES), 0)

    def row_of(k):
        y, s = divmod(k, DAYS)
        ahead = (count_ref[y, 0, s] < 0).astype(jnp.int32)
        return pl.multiple_of((s + ahead) * WIDE, 8)

    def cut_share():
        year = lax.axis_index("year")
        cells = share.shape[2]
        tiles = pl.cdiv(cells, LANES)
        part = cells % LANES
        for quarter in range(LANES // part):

            @pl.when(year % (LANES // part) == quarter)
            def _():
                start = year * cells - quarter * part
                span = pl.ds(pl.multiple_of(start, LANES), tiles * LANES)
                for e in range(DAYS):
                    row = by_hour[e, :, span]
                    cut[e] = row[:, quarter * part : quarter * part + cells].astype(jnp.bfloat16)

    stores = []
    body = STRIP - STRIP % 8
    for g in range(groups):
        for pair in range(g * GROUP, (g + 1) * GROUP):
            start = pair * 2 * STRIP
            even = row_of(2 * pair)
            odd = row_of(2 * pair + 1)

            def put(offset, size, value):
                span = pl.ds(start + offset, size)
                ready[span, :] = (field[span, :].astype(jnp.float32) - value).astype(jnp.bfloat16)

            put(0, body, climate[pl.ds(even, body), :])
            middle = jnp.where(
                sublane < 4,
                climate[pl.ds(even + body, 8), :],
                pltpu.roll(climate[pl.ds(odd, 8), :], 4, 0),
            )
            put(body, 8, middle)
            put(body + 8, body, climate[pl.ds(odd + 4, body), :])
        store = pltpu.make_async_copy(
            ready.at[pl.ds(g * size, size)], out.at[pl.ds(g * size, size)], store_sem.at[g]
        )
        store.start()
        stores.append(store)
        if g == groups // 2:
            cut_share()
            stores.append(pltpu.make_async_copy(cut, share, store_sem.at[groups]))
            stores[-1].start()
    for store in stores:
        store.wait()


def anomaly_of(field, counts, climate, cells):
    rows = YEARS * DAYS * STRIP
    groups = PAIRS // GROUP
    share = (DAYS, HOURS, cells)
    vmem = pl.BlockSpec(memory_space=pltpu.VMEM)
    return pl.pallas_call(
        subtract_kernel,
        out_shape=(
            jax.ShapeDtypeStruct((rows, LANES), jnp.bfloat16),
            jax.ShapeDtypeStruct(share, jnp.bfloat16),
        ),
        in_specs=[pl.BlockSpec(memory_space=pltpu.SMEM), vmem, vmem, vmem],
        out_specs=[pl.BlockSpec(memory_space=pltpu.HBM)] * 2,
        scratch_shapes=[
            pltpu.VMEM((rows, LANES), jnp.bfloat16),
            pltpu.VMEM(share, jnp.bfloat16),
            pltpu.SemaphoreType.DMA((groups + 1,)),
        ],
        compiler_params=pltpu.CompilerParams(vmem_limit_bytes=40 * 2**20),
        name="anomaly",
    )(counts, tile_rows(field), tile_rows(climate), climate)


def tile_rows(array):
    *lead, hours, cells = array.shape
    tiles = cells // LANES
    split = array.reshape(-1, hours, tiles, LANES)
    split = with_layout_constraint(split, Layout(major_to_minor=(0, 2, 1, 3)))
    return split.transpose(0, 2, 1, 3).reshape(-1, LANES)


def from_tile_rows(rows, shape):
    *lead, hours, cells = shape
    tiles = cells // LANES
    split = rows.reshape(-1, tiles, hours, LANES).transpose(0, 2, 1, 3)
    split = with_layout_constraint(split, Layout(major_to_minor=(0, 2, 1, 3)))
    return split.reshape(shape)


def local(field, day_index, sample_count):
    slot = lax.broadcasted_iota(jnp.int32, sample_count.shape, 1) + lax.axis_index("day") * DAYS
    counts = jnp.where(day_index[:, :, None] != slot, -sample_count, sample_count)
    counts = jnp.transpose(counts, (0, 2, 1))
    climate, field = climate_of(field, counts)
    cells = TILES * LANES // lax.axis_size("year")
    anomaly, share = anomaly_of(field, counts, climate, cells)
    return from_tile_rows(anomaly, field.shape), share


def solution(mesh):
    return jax.shard_map(
        local,
        mesh=mesh,
        in_specs=(P("year", "day", None, None), P("year", "day"), P("year", "day", None)),
        out_specs=(P("year", "day", None, None), P("day", None, "year")),
        check_vma=False,
    )
```

```python
import functools

import jax
import jax.numpy as jnp
from jax import lax
from jax.experimental import pallas as pl
from jax.experimental.layout import Layout, with_layout_constraint
from jax.experimental.pallas import tpu as pltpu
from jax.sharding import PartitionSpec as P

MESH = pl.DeviceIdType.MESH
HALF = 30
YEARS, DAYS, HOURS, TILES = 4, 23, 2, 90
LANES = 128
ROWS = DAYS + 1
MID = ROWS // 2
SLOT = 23
GROUPS = ((7, 4), (6, 6))
EDGE = ROWS // 3
MESSAGES = 8 + 44 * len(GROUPS)


def lanes(start, tiles):
    if isinstance(start, int):
        return pl.ds(start * LANES, tiles * LANES)
    return pl.ds(pl.multiple_of(start * LANES, LANES), tiles * LANES)


def rows_of(low):
    return pl.ds(0, MID) if low else pl.ds(MID, MID)


def shares(group):
    first, second = group
    return (first + 1) // 2, first // 2, second // 2


def reduce_kernel(
    field, count_ref, cl, held, part, weight, first_count, second_count,
    count0, count1, count2, count_x, count_z, count_d, kept, inverse, load_sem, send_sem, recv_sem,
    *buffers,
):
    day = lax.axis_index("day")
    year = lax.axis_index("year")
    days = lax.axis_size("day")
    z, u = year // 2, year % 2
    up, down, across = (z + 1) % 4, (z + 3) % 4, (z + 2) % 4
    at_up, at_down, at_across = (day, up * 2 + u), (day, down * 2 + u), (day, across * 2 + u)
    twin = (day, z * 2 + (1 - u))
    beside = [((day + step + days) % days, year) for step in (1, -1, 2, -2)]
    peers = [at_up, at_down, at_across, twin] + beside

    barrier = pltpu.get_barrier_semaphore()
    for peer in peers:
        pl.semaphore_signal(barrier, inc=1, device_id=peer, device_id_type=MESH)

    order = (across, up, down, z)
    inner = SLOT - 4 * SLOT + TILES
    loads = []
    for number, s in enumerate(order):
        span = lanes(s * SLOT, inner)
        loads.append((field.at[:, :, :, span], held.at[:, :, :, span], load_sem.at[number]))
    for s in range(3):
        span = lanes(s * SLOT + inner, SLOT - inner)
        loads.append((field.at[:, :, :, span], held.at[:, :, :, span], load_sem.at[4 + s]))
    loads = [pltpu.make_async_copy(*load) for load in loads]
    for load in loads[:1] + loads[4:] + loads[1:4]:
        load.start()

    used = []

    def copy(source, target, device):
        number = len(used)
        used.append(
            pltpu.make_async_remote_copy(
                src_ref=source, dst_ref=target, send_sem=send_sem.at[number],
                recv_sem=recv_sem.at[number], device_id=device, device_id_type=MESH,
            )
        )
        used[-1].start()
        return used[-1]

    total_own = jnp.zeros((HOURS, DAYS), jnp.float32)
    total_next = jnp.zeros((HOURS, DAYS), jnp.float32)
    for y in range(YEARS):
        counts = count_ref[y].astype(jnp.float32)
        own = jnp.maximum(counts, 0.0)
        after = jnp.maximum(-counts, 0.0)
        total_own += own
        total_next += after
        for s in range(DAYS):
            weight[y, s] = jnp.broadcast_to(own[:, s : s + 1], (HOURS, 4 * LANES))
            weight[y, DAYS + s] = jnp.broadcast_to(after[:, s : s + 1], (HOURS, 4 * LANES))
    first_count[...] = jnp.zeros_like(first_count)
    second_count[...] = jnp.zeros_like(second_count)
    first_count[:, :DAYS] = total_own
    second_count[:, :DAYS] = total_next
    count0[...] = first_count[...] + pltpu.roll(second_count[...], 1, 1)

    def add_years(start, tiles):
        halves = [(h, min(4, tiles - h)) for h in range(0, tiles, 4)]
        carried = [None] * len(halves)
        for s in range(DAYS):
            own = [None] * len(halves)
            after = [None] * len(halves)
            for y in range(YEARS):
                value = held[y, s, :, lanes(start, tiles)].astype(jnp.float32)
                for n, (h, width) in enumerate(halves):
                    piece = value[:, h * LANES : (h + width) * LANES]
                    a = piece * weight[y, s, :, : width * LANES]
                    b = piece * weight[y, DAYS + s, :, : width * LANES]
                    own[n] = a if y == 0 else own[n] + a
                    after[n] = b if y == 0 else after[n] + b
            for n, (h, width) in enumerate(halves):
                row = own[n] if s == 0 else own[n] + carried[n]
                part[s, :, lanes(start + h, width)] = row
            carried = after
        for n, (h, width) in enumerate(halves):
            part[DAYS, :, lanes(start + h, width)] = carried[n]

    part[:, :, TILES * LANES :] = jnp.zeros((ROWS, HOURS, (4 * SLOT - TILES) * LANES), jnp.float32)
    added = []

    def ready(number):
        while len(added) <= number:
            s = order[len(added)]
            for load in loads[:1] + loads[4:] if not added else loads[len(added) : len(added) + 1]:
                load.wait()
            start = s * SLOT

            @pl.loop(0, inner // 8)
            def _(step):
                add_years(start + step * 8, 8)

            add_years(start + inner // 8 * 8, inner % 8)

            @pl.when(s < 3)
            def _():
                add_years(start + inner, SLOT - inner)

            added.append(s)

    ready(0)
    pl.semaphore_wait(barrier, len(peers))

    class Ring:
        def __init__(self, buffers, at, tiles):
            self.buffers, self.at, self.tiles = buffers, at, tiles

        def piece(self, low, s):
            return part.at[rows_of(low), :, lanes(self.at(s), self.tiles)]

        def begin(self):
            ready(0)
            self.far_up = copy(self.piece(True, across), self.buffers.at[0], at_up)
            self.far_down = copy(self.piece(False, across), self.buffers.at[1], at_down)

        def near_up(self):
            ready(1)
            self.up = copy(self.piece(False, up), self.buffers.at[2], at_up)

        def near_down(self):
            ready(2)
            self.down = copy(self.piece(True, down), self.buffers.at[3], at_down)

        def forward(self):
            ready(2)
            self.far_up.wait_recv()
            self.add(True, up, 0)
            self.on_up = copy(self.piece(True, up), self.buffers.at[4], at_up)
            self.far_down.wait_recv()
            self.add(False, down, 1)
            self.on_down = copy(self.piece(False, down), self.buffers.at[5], at_down)

        def add(self, low, s, number):
            where = (rows_of(low), slice(None), lanes(self.at(s), self.tiles))
            part[where] = part[where] + self.buffers[number]

        def straight(self):
            ready(2)
            self.far_up = copy(self.piece(True, across), self.buffers.at[0], at_across)
            self.far_down = copy(self.piece(False, across), self.buffers.at[1], at_across)
            self.up = copy(self.piece(False, up), self.buffers.at[2], at_up)
            self.down = copy(self.piece(True, down), self.buffers.at[3], at_down)
            self.on_up = copy(self.piece(True, up), self.buffers.at[4], at_up)
            self.on_down = copy(self.piece(False, down), self.buffers.at[5], at_down)

        def straight_result(self):
            self.far_up.wait_recv()
            self.far_down.wait_recv()
            low, high = self.result()
            return low + self.buffers[0], high + self.buffers[1]

        def result(self):
            ready(3)
            self.up.wait_recv()
            self.down.wait_recv()
            self.on_up.wait_recv()
            self.on_down.wait_recv()
            where = lanes(self.at(z), self.tiles)
            low = part[rows_of(True), :, where] + self.buffers[3] + self.buffers[4]
            high = part[rows_of(False), :, where] + self.buffers[2] + self.buffers[5]
            return low, high

    class Spread:
        def __init__(self, at, tiles):
            self.at, self.tiles, self.forwarded = at, tiles, False

        def send(self, low, s, device):
            piece = cl.at[rows_of(low), :, lanes(self.at(s), self.tiles)]
            return copy(piece, piece, device)

        def begin(self, straight=False):
            if straight:
                self.up2 = self.send(True, z, at_across)
                self.down2 = self.send(False, z, at_across)
            self.up0 = self.send(True, z, at_up)
            self.down0 = self.send(False, z, at_down)
            self.up1 = self.send(False, z, at_up)
            self.down1 = self.send(True, z, at_down)

        def forward(self):
            self.forwarded = True
            self.up0.wait_recv()
            self.up2 = self.send(True, down, at_up)
            self.down0.wait_recv()
            self.down2 = self.send(False, up, at_down)

        def near(self):
            self.up1.wait_recv()
            self.down1.wait_recv()

        def near_all(self):
            if not self.forwarded:
                self.up0.wait_recv()
                self.down0.wait_recv()
            self.near()

        def far(self):
            self.up2.wait_recv()
            self.down2.wait_recv()

    class Group:
        def __init__(self, number):
            self.first, self.second = GROUPS[number]
            start = sum(map(sum, GROUPS[:number]))
            self.share, self.stride, self.half = shares(GROUPS[number])
            first_in, second_in, self.second_x, self.first_x, self.own, self.window = buffers[
                6 * number : 6 * number + 6
            ]
            self.first_at = lambda s: s * SLOT + start
            self.second_at = lambda s: s * SLOT + start + self.first
            self.kept_at = lambda s: self.second_at(s) + u * self.half
            self.ring = Ring(first_in, self.first_at, self.first)
            self.late_ring = Ring(second_in, self.kept_at, self.half)
            self.own_spread = Spread(lambda s: self.first_at(s) + u * self.stride, self.share)
            self.other_spread = Spread(
                lambda s: self.first_at(s) + (1 - u) * self.share, self.stride
            )
            self.late_spread = Spread(self.kept_at, self.half)
            self.swaps = []
            self.last = []

        def swap(self, *numbers):
            for number in numbers:
                ready(number)
                start = self.second_at(order[number]) + (1 - u) * self.half
                source = part.at[:, :, lanes(start, self.half)]
                self.swaps.append(copy(source, self.second_x.at[number], twin))

        def swapped(self, number):
            self.swaps[number].wait_recv()
            where = (slice(None), slice(None), lanes(self.kept_at(order[number]), self.half))
            part[where] = part[where] + self.second_x[number]

        def near(self):
            self.ring.near_up()
            self.ring.near_down()

        def late_begin(self):
            self.swapped(0)
            self.late_ring.begin()

        def late_straight(self):
            for number in range(3):
                self.swapped(number)
            self.late_ring.straight()

        def late_near(self):
            self.swapped(1)
            self.late_ring.near_up()
            self.swapped(2)
            self.late_ring.near_down()

        def swap_first(self):
            low, high = self.ring.result()
            where = lanes(self.first_at(z), self.first)
            part[rows_of(True), :, where] = low
            part[rows_of(False), :, where] = high
            start = self.first_at(z) + (1 - u) * self.stride
            self.pair = copy(part.at[:, :, lanes(start, self.share)], self.first_x, twin)

        def late_result(self, straight=False):
            self.swapped(3)
            low, high = self.late_ring.straight_result() if straight else self.late_ring.result()
            span = pl.ds(self.share * LANES, self.half * LANES)
            self.own[rows_of(True), :, span] = low
            self.own[rows_of(False), :, span] = high

        def share_out(self):
            self.pair.wait_recv()
            span = lanes(self.first_at(z) + u * self.stride, self.share)
            self.own[:, :, : self.share * LANES] = part[:, :, span] + self.first_x[...]
            right, left, right2, left2 = beside
            own, window = self.own, self.window
            self.out = [
                copy(own, window.at[pl.ds(0, ROWS)], right),
                copy(own, window.at[pl.ds(ROWS, ROWS)], left),
                copy(own.at[pl.ds(ROWS - EDGE, EDGE)], window.at[pl.ds(2 * ROWS, EDGE)], right2),
                copy(own.at[pl.ds(0, EDGE)], window.at[pl.ds(2 * ROWS + EDGE, EDGE)], left2),
            ]

        def smooth(self):
            for message in self.out:
                message.wait_recv()
            own, window = self.own, self.window

            def day_row(offset, span):
                if offset < -DAYS:
                    return window[2 * ROWS + offset + 2 * DAYS - (ROWS - EDGE), :, span]
                if offset == -DAYS:
                    return window[0, :, span] + window[2 * ROWS + EDGE - 1, :, span]
                if offset < 0:
                    return window[offset + DAYS, :, span]
                if offset == 0:
                    return own[0, :, span] + window[DAYS, :, span]
                if offset < DAYS:
                    return own[offset, :, span]
                if offset == DAYS:
                    return window[ROWS, :, span] + own[DAYS, :, span]
                if offset < 2 * DAYS:
                    return window[ROWS + offset - DAYS, :, span]
                if offset == 2 * DAYS:
                    return window[2 * ROWS + EDGE, :, span] + window[ROWS + DAYS, :, span]
                return window[2 * ROWS + EDGE + offset - 2 * DAYS, :, span]

            def smoothed(start, at, tiles):
                for h in range(0, tiles, 4):
                    width = min(4, tiles - h)
                    span = pl.ds((start + h) * LANES, width * LANES)
                    total = day_row(0, span)
                    for offset in range(1, DAYS):
                        total = total + day_row(offset, span)
                    for offset in range(-1, -HALF - 1, -1):
                        total = total + day_row(offset, span)
                        if offset + HALF < ROWS:
                            kept[offset + HALF, :, : width * LANES] = total
                    total = None
                    for offset in range(DAYS, DAYS + HALF + 1):
                        row = day_row(offset, span)
                        total = row if total is None else total + row
                        if offset >= HALF:
                            i = offset - HALF
                            sums = kept[i, :, : width * LANES] + total
                            scaled = sums * inverse[i, :, : width * LANES]
                            cl[i, :, lanes(at + h, width)] = scaled

            smoothed(0, self.first_at(z) + u * self.stride, self.share)
            smoothed(self.share, self.kept_at(z), self.half)

        def across_x(self, s):
            piece = cl.at[:, :, lanes(self.kept_at(s), self.half)]
            self.last.append(copy(piece, piece, twin))

        def spread_second(self, straight=False):
            self.late_spread.begin(straight)
            self.across_x(z)

        def spread_first(self):
            piece = cl.at[:, :, lanes(self.first_at(z) + u * self.share, self.stride)]
            self.pair = copy(piece, piece, twin)
            self.own_spread.begin()

        def late_forward(self):
            self.late_spread.forward()

        def late_across(self):
            self.late_spread.near()
            self.across_x(up)
            self.across_x(down)

        def other(self, straight=False):
            self.pair.wait_recv()
            self.other_spread.begin(straight)

        def late_far(self):
            self.late_spread.far()
            self.across_x(across)

        def end(self):
            for portion in (self.own_spread, self.other_spread):
                portion.near_all()
                portion.far()
            for message in self.last:
                message.wait_recv()

    def windows():
        for message in aside:
            message.wait_recv()
        spread = (
            count_d[2]
            + pltpu.roll(count_d[0], DAYS, 1)
            + pltpu.roll(count2[...], 2 * DAYS, 1)
            + pltpu.roll(count_d[1], 3 * DAYS, 1)
            + pltpu.roll(count_d[3], 4 * DAYS, 1)
        )
        lane = lax.broadcasted_iota(jnp.int32, (HOURS, LANES), 1)
        for i in range(ROWS):
            start = 2 * DAYS - HALF + i
            inside = (lane >= start) & (lane <= start + 2 * HALF)
            count = jnp.sum(jnp.where(inside, spread, 0.0), axis=1, keepdims=True)
            inverse[i] = jnp.broadcast_to(1.0 / count, (HOURS, 4 * LANES))

    send_count = copy(count0, count_x, twin)
    one, two = (Group(number) for number in range(len(GROUPS)))
    one.ring.begin()
    two.swap(0)
    one.swap(0)
    two.swap(1)
    one.swap(1, 2)
    two.ring.begin()
    two.swap(2)
    one.near()
    send_count.wait_recv()
    count1[...] = count0[...] + count_x[...]
    along = [copy(count1, count_z.at[n], d) for n, d in enumerate((at_up, at_down, at_across))]
    one.ring.forward()
    one.late_begin()
    two.ring.forward()
    one.swap(3)
    two.near()
    one.swap_first()
    one.late_near()
    two.swap(3)
    one.late_ring.forward()
    two.late_begin()
    two.swap_first()
    one.late_result()
    two.late_near()
    for message in along:
        message.wait_recv()
    count2[...] = count1[...] + count_z[0] + count_z[1] + count_z[2]
    aside = [copy(count2, count_d.at[n], d) for n, d in enumerate(beside)]
    one.share_out()
    two.late_ring.forward()
    two.late_result()
    two.share_out()
    windows()
    one.smooth()
    one.spread_second()
    one.spread_first()
    two.smooth()
    two.spread_second()
    one.late_forward()
    two.spread_first()
    one.late_across()
    two.late_forward()
    two.late_across()
    one.other()
    one.late_far()
    two.own_spread.forward()
    two.other(straight=True)
    two.late_far()
    one.own_spread.forward()
    one.other_spread.forward()
    for group in (one, two):
        group.end()
    for message in used:
        message.wait_send()


def climate_of(field, counts):
    f32 = jnp.float32
    wide = 4 * SLOT * LANES
    vmem = pltpu.VMEM
    row = (HOURS, LANES)
    scratch = [
        vmem((ROWS, HOURS, wide), f32),
        vmem((YEARS, 2 * DAYS, HOURS, 4 * LANES), f32),
        vmem(row, f32), vmem(row, f32), vmem(row, f32), vmem(row, f32), vmem(row, f32),
        vmem(row, f32), vmem((3, *row), f32), vmem((4, *row), f32),
        vmem((ROWS, HOURS, 4 * LANES), f32),
        vmem((ROWS, HOURS, 4 * LANES), f32),
        pltpu.SemaphoreType.DMA((7,)),
        pltpu.SemaphoreType.DMA((MESSAGES,)),
        pltpu.SemaphoreType.DMA((MESSAGES,)),
    ]
    for group in GROUPS:
        share, _, half = shares(group)
        together = (share + half) * LANES
        scratch += [
            vmem((6, MID, HOURS, group[0] * LANES), f32),
            vmem((6, MID, HOURS, half * LANES), f32),
            vmem((4, ROWS, HOURS, half * LANES), f32),
            vmem((ROWS, HOURS, share * LANES), f32),
            vmem((ROWS, HOURS, together), f32),
            vmem((2 * ROWS + 2 * EDGE, HOURS, together), f32),
        ]
    return pl.pallas_call(
        reduce_kernel,
        out_shape=(
            jax.ShapeDtypeStruct((ROWS, HOURS, wide), f32),
            jax.ShapeDtypeStruct(field.shape, field.dtype),
        ),
        in_specs=[
            pl.BlockSpec(memory_space=pltpu.HBM),
            pl.BlockSpec(memory_space=vmem),
        ],
        out_specs=[pl.BlockSpec(memory_space=vmem)] * 2,
        scratch_shapes=scratch,
        compiler_params=pltpu.CompilerParams(
            collective_id=0, has_side_effects=True, vmem_limit_bytes=46 * 2**20
        ),
        name="climate",
    )(field, counts)


STRIP = HOURS * TILES
WIDE = HOURS * 4 * SLOT
PAIRS = YEARS * DAYS // 2
GROUP = 2


def subtract_kernel(count_ref, field, climate, by_hour, out, share, ready, cut, store_sem):
    size = GROUP * 2 * STRIP
    groups = PAIRS // GROUP
    sublane = lax.broadcasted_iota(jnp.int32, (8, LANES), 0)

    def row_of(k):
        y, s = divmod(k, DAYS)
        ahead = (count_ref[y, 0, s] < 0).astype(jnp.int32)
        return pl.multiple_of((s + ahead) * WIDE, 8)

    def cut_share():
        year = lax.axis_index("year")
        cells = share.shape[2]
        tiles = pl.cdiv(cells, LANES)
        part = cells % LANES
        for quarter in range(LANES // part):

            @pl.when(year % (LANES // part) == quarter)
            def _():
                start = year * cells - quarter * part
                span = pl.ds(pl.multiple_of(start, LANES), tiles * LANES)
                for e in range(DAYS):
                    row = by_hour[e, :, span]
                    cut[e] = row[:, quarter * part : quarter * part + cells].astype(jnp.bfloat16)

    stores = []
    body = STRIP - STRIP % 8
    for g in range(groups):
        for pair in range(g * GROUP, (g + 1) * GROUP):
            start = pair * 2 * STRIP
            even = row_of(2 * pair)
            odd = row_of(2 * pair + 1)

            def put(offset, size, value):
                span = pl.ds(start + offset, size)
                ready[span, :] = (field[span, :].astype(jnp.float32) - value).astype(jnp.bfloat16)

            put(0, body, climate[pl.ds(even, body), :])
            middle = jnp.where(
                sublane < 4,
                climate[pl.ds(even + body, 8), :],
                pltpu.roll(climate[pl.ds(odd, 8), :], 4, 0),
            )
            put(body, 8, middle)
            put(body + 8, body, climate[pl.ds(odd + 4, body), :])
        store = pltpu.make_async_copy(
            ready.at[pl.ds(g * size, size)], out.at[pl.ds(g * size, size)], store_sem.at[g]
        )
        store.start()
        stores.append(store)
        if g == groups // 2:
            cut_share()
            stores.append(pltpu.make_async_copy(cut, share, store_sem.at[groups]))
            stores[-1].start()
    for store in stores:
        store.wait()


def anomaly_of(field, counts, climate, cells):
    rows = YEARS * DAYS * STRIP
    groups = PAIRS // GROUP
    share = (DAYS, HOURS, cells)
    vmem = pl.BlockSpec(memory_space=pltpu.VMEM)
    return pl.pallas_call(
        subtract_kernel,
        out_shape=(
            jax.ShapeDtypeStruct((rows, LANES), jnp.bfloat16),
            jax.ShapeDtypeStruct(share, jnp.bfloat16),
        ),
        in_specs=[pl.BlockSpec(memory_space=pltpu.SMEM), vmem, vmem, vmem],
        out_specs=[pl.BlockSpec(memory_space=pltpu.HBM)] * 2,
        scratch_shapes=[
            pltpu.VMEM((rows, LANES), jnp.bfloat16),
            pltpu.VMEM(share, jnp.bfloat16),
            pltpu.SemaphoreType.DMA((groups + 1,)),
        ],
        compiler_params=pltpu.CompilerParams(vmem_limit_bytes=40 * 2**20),
        name="anomaly",
    )(counts, tile_rows(field), tile_rows(climate), climate)


def tile_rows(array):
    *lead, hours, cells = array.shape
    tiles = cells // LANES
    split = array.reshape(-1, hours, tiles, LANES)
    split = with_layout_constraint(split, Layout(major_to_minor=(0, 2, 1, 3)))
    return split.transpose(0, 2, 1, 3).reshape(-1, LANES)


def from_tile_rows(rows, shape):
    *lead, hours, cells = shape
    tiles = cells // LANES
    split = rows.reshape(-1, tiles, hours, LANES).transpose(0, 2, 1, 3)
    split = with_layout_constraint(split, Layout(major_to_minor=(0, 2, 1, 3)))
    return split.reshape(shape)


def local(field, day_index, sample_count):
    slot = lax.broadcasted_iota(jnp.int32, sample_count.shape, 1) + lax.axis_index("day") * DAYS
    counts = jnp.where(day_index[:, :, None] != slot, -sample_count, sample_count)
    counts = jnp.transpose(counts, (0, 2, 1))
    climate, field = climate_of(field, counts)
    cells = TILES * LANES // lax.axis_size("year")
    anomaly, share = anomaly_of(field, counts, climate, cells)
    return from_tile_rows(anomaly, field.shape), share


def solution(mesh):
    return jax.shard_map(
        local,
        mesh=mesh,
        in_specs=(P("year", "day", None, None), P("year", "day"), P("year", "day", None)),
        out_specs=(P("year", "day", None, None), P("day", None, "year")),
        check_vma=False,
    )
```

```python
import functools

import jax
import jax.numpy as jnp
from jax import lax
from jax.experimental import pallas as pl
from jax.experimental.layout import Layout, with_layout_constraint
from jax.experimental.pallas import tpu as pltpu
from jax.sharding import PartitionSpec as P

MESH = pl.DeviceIdType.MESH
HALF = 30
YEARS, DAYS, HOURS, TILES = 4, 23, 2, 90
LANES = 128
ROWS = DAYS + 1
MID = ROWS // 2
SLOT = 23
GROUPS = ((7, 4), (6, 6))
EDGE = ROWS // 3
MESSAGES = 8 + 44 * len(GROUPS)


def lanes(start, tiles):
    if isinstance(start, int):
        return pl.ds(start * LANES, tiles * LANES)
    return pl.ds(pl.multiple_of(start * LANES, LANES), tiles * LANES)


def rows_of(low):
    return pl.ds(0, MID) if low else pl.ds(MID, MID)


def shares(group):
    first, second = group
    return (first + 1) // 2, first // 2, second // 2


def reduce_kernel(
    field, count_ref, cl, held, part, weight, first_count, second_count,
    count0, count1, count2, count_x, count_z, count_d, kept, inverse, load_sem, send_sem, recv_sem,
    *buffers,
):
    day = lax.axis_index("day")
    year = lax.axis_index("year")
    days = lax.axis_size("day")
    z, u = year // 2, year % 2
    up, down, across = (z + 1) % 4, (z + 3) % 4, (z + 2) % 4
    at_up, at_down, at_across = (day, up * 2 + u), (day, down * 2 + u), (day, across * 2 + u)
    twin = (day, z * 2 + (1 - u))
    beside = [((day + step + days) % days, year) for step in (1, -1, 2, -2)]
    peers = [at_up, at_down, at_across, twin] + beside

    barrier = pltpu.get_barrier_semaphore()
    for peer in peers:
        pl.semaphore_signal(barrier, inc=1, device_id=peer, device_id_type=MESH)

    order = (across, up, down, z)
    inner = SLOT - 4 * SLOT + TILES
    loads = []
    for number, s in enumerate(order):
        span = lanes(s * SLOT, inner)
        loads.append((field.at[:, :, :, span], held.at[:, :, :, span], load_sem.at[number]))
    for s in range(3):
        span = lanes(s * SLOT + inner, SLOT - inner)
        loads.append((field.at[:, :, :, span], held.at[:, :, :, span], load_sem.at[4 + s]))
    loads = [pltpu.make_async_copy(*load) for load in loads]
    for load in loads[:1] + loads[4:] + loads[1:4]:
        load.start()

    used = []

    def copy(source, target, device):
        number = len(used)
        used.append(
            pltpu.make_async_remote_copy(
                src_ref=source, dst_ref=target, send_sem=send_sem.at[number],
                recv_sem=recv_sem.at[number], device_id=device, device_id_type=MESH,
            )
        )
        used[-1].start()
        return used[-1]

    total_own = jnp.zeros((HOURS, DAYS), jnp.float32)
    total_next = jnp.zeros((HOURS, DAYS), jnp.float32)
    for y in range(YEARS):
        counts = count_ref[y].astype(jnp.float32)
        own = jnp.maximum(counts, 0.0)
        after = jnp.maximum(-counts, 0.0)
        total_own += own
        total_next += after
        for s in range(DAYS):
            weight[y, s] = jnp.broadcast_to(own[:, s : s + 1], (HOURS, 4 * LANES))
            weight[y, DAYS + s] = jnp.broadcast_to(after[:, s : s + 1], (HOURS, 4 * LANES))
    first_count[...] = jnp.zeros_like(first_count)
    second_count[...] = jnp.zeros_like(second_count)
    first_count[:, :DAYS] = total_own
    second_count[:, :DAYS] = total_next
    count0[...] = first_count[...] + pltpu.roll(second_count[...], 1, 1)

    def add_years(start, tiles):
        halves = [(h, min(4, tiles - h)) for h in range(0, tiles, 4)]
        carried = [None] * len(halves)
        for s in range(DAYS):
            own = [None] * len(halves)
            after = [None] * len(halves)
            for y in range(YEARS):
                value = held[y, s, :, lanes(start, tiles)].astype(jnp.float32)
                for n, (h, width) in enumerate(halves):
                    piece = value[:, h * LANES : (h + width) * LANES]
                    a = piece * weight[y, s, :, : width * LANES]
                    b = piece * weight[y, DAYS + s, :, : width * LANES]
                    own[n] = a if y == 0 else own[n] + a
                    after[n] = b if y == 0 else after[n] + b
            for n, (h, width) in enumerate(halves):
                row = own[n] if s == 0 else own[n] + carried[n]
                part[s, :, lanes(start + h, width)] = row
            carried = after
        for n, (h, width) in enumerate(halves):
            part[DAYS, :, lanes(start + h, width)] = carried[n]

    part[:, :, TILES * LANES :] = jnp.zeros((ROWS, HOURS, (4 * SLOT - TILES) * LANES), jnp.float32)
    added = []

    def ready(number):
        while len(added) <= number:
            s = order[len(added)]
            for load in loads[:1] + loads[4:] if not added else loads[len(added) : len(added) + 1]:
                load.wait()
            start = s * SLOT

            @pl.loop(0, inner // 8)
            def _(step):
                add_years(start + step * 8, 8)

            add_years(start + inner // 8 * 8, inner % 8)

            @pl.when(s < 3)
            def _():
                add_years(start + inner, SLOT - inner)

            added.append(s)

    ready(0)
    pl.semaphore_wait(barrier, len(peers))

    class Ring:
        def __init__(self, buffers, at, tiles):
            self.buffers, self.at, self.tiles = buffers, at, tiles

        def piece(self, low, s):
            return part.at[rows_of(low), :, lanes(self.at(s), self.tiles)]

        def begin(self):
            ready(0)
            self.far_up = copy(self.piece(True, across), self.buffers.at[0], at_up)
            self.far_down = copy(self.piece(False, across), self.buffers.at[1], at_down)

        def near_up(self):
            ready(1)
            self.up = copy(self.piece(False, up), self.buffers.at[2], at_up)

        def near_down(self):
            ready(2)
            self.down = copy(self.piece(True, down), self.buffers.at[3], at_down)

        def forward(self):
            ready(2)
            self.far_up.wait_recv()
            self.add(True, up, 0)
            self.on_up = copy(self.piece(True, up), self.buffers.at[4], at_up)
            self.far_down.wait_recv()
            self.add(False, down, 1)
            self.on_down = copy(self.piece(False, down), self.buffers.at[5], at_down)

        def add(self, low, s, number):
            where = (rows_of(low), slice(None), lanes(self.at(s), self.tiles))
            part[where] = part[where] + self.buffers[number]

        def straight(self):
            ready(2)
            self.far_up = copy(self.piece(True, across), self.buffers.at[0], at_across)
            self.far_down = copy(self.piece(False, across), self.buffers.at[1], at_across)
            self.up = copy(self.piece(False, up), self.buffers.at[2], at_up)
            self.down = copy(self.piece(True, down), self.buffers.at[3], at_down)
            self.on_up = copy(self.piece(True, up), self.buffers.at[4], at_up)
            self.on_down = copy(self.piece(False, down), self.buffers.at[5], at_down)

        def straight_result(self):
            self.far_up.wait_recv()
            self.far_down.wait_recv()
            low, high = self.result()
            return low + self.buffers[0], high + self.buffers[1]

        def result(self):
            ready(3)
            self.up.wait_recv()
            self.down.wait_recv()
            self.on_up.wait_recv()
            self.on_down.wait_recv()
            where = lanes(self.at(z), self.tiles)
            low = part[rows_of(True), :, where] + self.buffers[3] + self.buffers[4]
            high = part[rows_of(False), :, where] + self.buffers[2] + self.buffers[5]
            return low, high

    class Spread:
        def __init__(self, at, tiles):
            self.at, self.tiles, self.forwarded = at, tiles, False

        def send(self, low, s, device):
            piece = cl.at[rows_of(low), :, lanes(self.at(s), self.tiles)]
            return copy(piece, piece, device)

        def begin(self, straight=False):
            if straight:
                self.up2 = self.send(True, z, at_across)
                self.down2 = self.send(False, z, at_across)
            self.up0 = self.send(True, z, at_up)
            self.down0 = self.send(False, z, at_down)
            self.up1 = self.send(False, z, at_up)
            self.down1 = self.send(True, z, at_down)

        def forward(self):
            self.forwarded = True
            self.up0.wait_recv()
            self.up2 = self.send(True, down, at_up)
            self.down0.wait_recv()
            self.down2 = self.send(False, up, at_down)

        def near(self):
            self.up1.wait_recv()
            self.down1.wait_recv()

        def near_all(self):
            if not self.forwarded:
                self.up0.wait_recv()
                self.down0.wait_recv()
            self.near()

        def far(self):
            self.up2.wait_recv()
            self.down2.wait_recv()

    class Group:
        def __init__(self, number):
            self.first, self.second = GROUPS[number]
            start = sum(map(sum, GROUPS[:number]))
            self.share, self.stride, self.half = shares(GROUPS[number])
            first_in, second_in, self.second_x, self.first_x, self.own, self.window = buffers[
                6 * number : 6 * number + 6
            ]
            self.first_at = lambda s: s * SLOT + start
            self.second_at = lambda s: s * SLOT + start + self.first
            self.kept_at = lambda s: self.second_at(s) + u * self.half
            self.ring = Ring(first_in, self.first_at, self.first)
            self.late_ring = Ring(second_in, self.kept_at, self.half)
            self.own_spread = Spread(lambda s: self.first_at(s) + u * self.stride, self.share)
            self.other_spread = Spread(
                lambda s: self.first_at(s) + (1 - u) * self.share, self.stride
            )
            self.late_spread = Spread(self.kept_at, self.half)
            self.swaps = []
            self.last = []

        def swap(self, *numbers):
            for number in numbers:
                ready(number)
                start = self.second_at(order[number]) + (1 - u) * self.half
                source = part.at[:, :, lanes(start, self.half)]
                self.swaps.append(copy(source, self.second_x.at[number], twin))

        def swapped(self, number):
            self.swaps[number].wait_recv()
            where = (slice(None), slice(None), lanes(self.kept_at(order[number]), self.half))
            part[where] = part[where] + self.second_x[number]

        def near(self):
            self.ring.near_up()
            self.ring.near_down()

        def late_begin(self):
            self.swapped(0)
            self.late_ring.begin()

        def late_straight(self):
            for number in range(3):
                self.swapped(number)
            self.late_ring.straight()

        def late_near(self):
            self.swapped(1)
            self.late_ring.near_up()
            self.swapped(2)
            self.late_ring.near_down()

        def swap_first(self):
            low, high = self.ring.result()
            where = lanes(self.first_at(z), self.first)
            part[rows_of(True), :, where] = low
            part[rows_of(False), :, where] = high
            start = self.first_at(z) + (1 - u) * self.stride
            self.pair = copy(part.at[:, :, lanes(start, self.share)], self.first_x, twin)

        def late_result(self, straight=False):
            self.swapped(3)
            low, high = self.late_ring.straight_result() if straight else self.late_ring.result()
            span = pl.ds(self.share * LANES, self.half * LANES)
            self.own[rows_of(True), :, span] = low
            self.own[rows_of(False), :, span] = high

        def share_out(self):
            self.pair.wait_recv()
            span = lanes(self.first_at(z) + u * self.stride, self.share)
            self.own[:, :, : self.share * LANES] = part[:, :, span] + self.first_x[...]
            right, left, right2, left2 = beside
            own, window = self.own, self.window
            self.out = [
                copy(own, window.at[pl.ds(0, ROWS)], right),
                copy(own, window.at[pl.ds(ROWS, ROWS)], left),
                copy(own.at[pl.ds(ROWS - EDGE, EDGE)], window.at[pl.ds(2 * ROWS, EDGE)], right2),
                copy(own.at[pl.ds(0, EDGE)], window.at[pl.ds(2 * ROWS + EDGE, EDGE)], left2),
            ]

        def smooth(self):
            for message in self.out:
                message.wait_recv()
            own, window = self.own, self.window

            def day_row(offset, span):
                if offset < -DAYS:
                    return window[2 * ROWS + offset + 2 * DAYS - (ROWS - EDGE), :, span]
                if offset == -DAYS:
                    return window[0, :, span] + window[2 * ROWS + EDGE - 1, :, span]
                if offset < 0:
                    return window[offset + DAYS, :, span]
                if offset == 0:
                    return own[0, :, span] + window[DAYS, :, span]
                if offset < DAYS:
                    return own[offset, :, span]
                if offset == DAYS:
                    return window[ROWS, :, span] + own[DAYS, :, span]
                if offset < 2 * DAYS:
                    return window[ROWS + offset - DAYS, :, span]
                if offset == 2 * DAYS:
                    return window[2 * ROWS + EDGE, :, span] + window[ROWS + DAYS, :, span]
                return window[2 * ROWS + EDGE + offset - 2 * DAYS, :, span]

            def smoothed(start, at, tiles):
                for h in range(0, tiles, 4):
                    width = min(4, tiles - h)
                    span = pl.ds((start + h) * LANES, width * LANES)
                    total = day_row(0, span)
                    for offset in range(1, DAYS):
                        total = total + day_row(offset, span)
                    for offset in range(-1, -HALF - 1, -1):
                        total = total + day_row(offset, span)
                        if offset + HALF < ROWS:
                            kept[offset + HALF, :, : width * LANES] = total
                    total = None
                    for offset in range(DAYS, DAYS + HALF + 1):
                        row = day_row(offset, span)
                        total = row if total is None else total + row
                        if offset >= HALF:
                            i = offset - HALF
                            sums = kept[i, :, : width * LANES] + total
                            scaled = sums * inverse[i, :, : width * LANES]
                            cl[i, :, lanes(at + h, width)] = scaled

            smoothed(0, self.first_at(z) + u * self.stride, self.share)
            smoothed(self.share, self.kept_at(z), self.half)

        def across_x(self, s):
            piece = cl.at[:, :, lanes(self.kept_at(s), self.half)]
            self.last.append(copy(piece, piece, twin))

        def spread_second(self, straight=False):
            self.late_spread.begin(straight)
            self.across_x(z)

        def spread_first(self):
            piece = cl.at[:, :, lanes(self.first_at(z) + u * self.share, self.stride)]
            self.pair = copy(piece, piece, twin)
            self.own_spread.begin()

        def late_forward(self):
            self.late_spread.forward()

        def late_across(self):
            self.late_spread.near()
            self.across_x(up)
            self.across_x(down)

        def other(self, straight=False):
            self.pair.wait_recv()
            self.other_spread.begin(straight)

        def late_far(self):
            self.late_spread.far()
            self.across_x(across)

        def end(self):
            for portion in (self.own_spread, self.other_spread):
                portion.near_all()
                portion.far()
            for message in self.last:
                message.wait_recv()

    def windows():
        for message in aside:
            message.wait_recv()
        spread = (
            count_d[2]
            + pltpu.roll(count_d[0], DAYS, 1)
            + pltpu.roll(count2[...], 2 * DAYS, 1)
            + pltpu.roll(count_d[1], 3 * DAYS, 1)
            + pltpu.roll(count_d[3], 4 * DAYS, 1)
        )
        lane = lax.broadcasted_iota(jnp.int32, (HOURS, LANES), 1)
        for i in range(ROWS):
            start = 2 * DAYS - HALF + i
            inside = (lane >= start) & (lane <= start + 2 * HALF)
            count = jnp.sum(jnp.where(inside, spread, 0.0), axis=1, keepdims=True)
            inverse[i] = jnp.broadcast_to(1.0 / count, (HOURS, 4 * LANES))

    send_count = copy(count0, count_x, twin)
    one, two = (Group(number) for number in range(len(GROUPS)))
    one.ring.begin()
    two.swap(0)
    one.swap(0)
    two.swap(1)
    one.swap(1, 2)
    two.ring.begin()
    two.swap(2)
    one.near()
    send_count.wait_recv()
    count1[...] = count0[...] + count_x[...]
    along = [copy(count1, count_z.at[n], d) for n, d in enumerate((at_up, at_down, at_across))]
    one.ring.forward()
    one.late_begin()
    two.ring.forward()
    one.swap(3)
    two.near()
    for message in along:
        message.wait_recv()
    count2[...] = count1[...] + count_z[0] + count_z[1] + count_z[2]
    aside = [copy(count2, count_d.at[n], d) for n, d in enumerate(beside)]
    one.swap_first()
    one.late_near()
    two.swap(3)
    one.late_ring.forward()
    two.late_begin()
    two.swap_first()
    one.late_result()
    two.late_near()
    one.share_out()
    two.late_ring.forward()
    windows()
    two.late_result()
    two.share_out()
    one.smooth()
    one.spread_second()
    one.spread_first()
    two.smooth()
    two.spread_second()
    one.late_forward()
    two.spread_first()
    one.late_across()
    two.late_forward()
    two.late_across()
    one.other()
    one.late_far()
    two.own_spread.forward()
    two.other(straight=True)
    two.late_far()
    one.own_spread.forward()
    one.other_spread.forward()
    for group in (one, two):
        group.end()
    for message in used:
        message.wait_send()


def climate_of(field, counts):
    f32 = jnp.float32
    wide = 4 * SLOT * LANES
    vmem = pltpu.VMEM
    row = (HOURS, LANES)
    scratch = [
        vmem((ROWS, HOURS, wide), f32),
        vmem((YEARS, 2 * DAYS, HOURS, 4 * LANES), f32),
        vmem(row, f32), vmem(row, f32), vmem(row, f32), vmem(row, f32), vmem(row, f32),
        vmem(row, f32), vmem((3, *row), f32), vmem((4, *row), f32),
        vmem((ROWS, HOURS, 4 * LANES), f32),
        vmem((ROWS, HOURS, 4 * LANES), f32),
        pltpu.SemaphoreType.DMA((7,)),
        pltpu.SemaphoreType.DMA((MESSAGES,)),
        pltpu.SemaphoreType.DMA((MESSAGES,)),
    ]
    for group in GROUPS:
        share, _, half = shares(group)
        together = (share + half) * LANES
        scratch += [
            vmem((6, MID, HOURS, group[0] * LANES), f32),
            vmem((6, MID, HOURS, half * LANES), f32),
            vmem((4, ROWS, HOURS, half * LANES), f32),
            vmem((ROWS, HOURS, share * LANES), f32),
            vmem((ROWS, HOURS, together), f32),
            vmem((2 * ROWS + 2 * EDGE, HOURS, together), f32),
        ]
    return pl.pallas_call(
        reduce_kernel,
        out_shape=(
            jax.ShapeDtypeStruct((ROWS, HOURS, wide), f32),
            jax.ShapeDtypeStruct(field.shape, field.dtype),
        ),
        in_specs=[
            pl.BlockSpec(memory_space=pltpu.HBM),
            pl.BlockSpec(memory_space=vmem),
        ],
        out_specs=[pl.BlockSpec(memory_space=vmem)] * 2,
        scratch_shapes=scratch,
        compiler_params=pltpu.CompilerParams(
            collective_id=0, has_side_effects=True, vmem_limit_bytes=46 * 2**20
        ),
        name="climate",
    )(field, counts)


STRIP = HOURS * TILES
WIDE = HOURS * 4 * SLOT
PAIRS = YEARS * DAYS // 2
GROUP = 2


def subtract_kernel(count_ref, field, climate, by_hour, out, share, ready, cut, store_sem):
    size = GROUP * 2 * STRIP
    groups = PAIRS // GROUP
    sublane = lax.broadcasted_iota(jnp.int32, (8, LANES), 0)

    def row_of(k):
        y, s = divmod(k, DAYS)
        ahead = (count_ref[y, 0, s] < 0).astype(jnp.int32)
        return pl.multiple_of((s + ahead) * WIDE, 8)

    def cut_share():
        year = lax.axis_index("year")
        cells = share.shape[2]
        tiles = pl.cdiv(cells, LANES)
        part = cells % LANES
        for quarter in range(LANES // part):

            @pl.when(year % (LANES // part) == quarter)
            def _():
                start = year * cells - quarter * part
                span = pl.ds(pl.multiple_of(start, LANES), tiles * LANES)
                for e in range(DAYS):
                    row = by_hour[e, :, span]
                    cut[e] = row[:, quarter * part : quarter * part + cells].astype(jnp.bfloat16)

    stores = []
    body = STRIP - STRIP % 8
    for g in range(groups):
        for pair in range(g * GROUP, (g + 1) * GROUP):
            start = pair * 2 * STRIP
            even = row_of(2 * pair)
            odd = row_of(2 * pair + 1)

            def put(offset, size, value):
                span = pl.ds(start + offset, size)
                ready[span, :] = (field[span, :].astype(jnp.float32) - value).astype(jnp.bfloat16)

            put(0, body, climate[pl.ds(even, body), :])
            middle = jnp.where(
                sublane < 4,
                climate[pl.ds(even + body, 8), :],
                pltpu.roll(climate[pl.ds(odd, 8), :], 4, 0),
            )
            put(body, 8, middle)
            put(body + 8, body, climate[pl.ds(odd + 4, body), :])
        store = pltpu.make_async_copy(
            ready.at[pl.ds(g * size, size)], out.at[pl.ds(g * size, size)], store_sem.at[g]
        )
        store.start()
        stores.append(store)
        if g == groups // 2:
            cut_share()
            stores.append(pltpu.make_async_copy(cut, share, store_sem.at[groups]))
            stores[-1].start()
    for store in stores:
        store.wait()


def anomaly_of(field, counts, climate, cells):
    rows = YEARS * DAYS * STRIP
    groups = PAIRS // GROUP
    share = (DAYS, HOURS, cells)
    vmem = pl.BlockSpec(memory_space=pltpu.VMEM)
    return pl.pallas_call(
        subtract_kernel,
        out_shape=(
            jax.ShapeDtypeStruct((rows, LANES), jnp.bfloat16),
            jax.ShapeDtypeStruct(share, jnp.bfloat16),
        ),
        in_specs=[pl.BlockSpec(memory_space=pltpu.SMEM), vmem, vmem, vmem],
        out_specs=[pl.BlockSpec(memory_space=pltpu.HBM)] * 2,
        scratch_shapes=[
            pltpu.VMEM((rows, LANES), jnp.bfloat16),
            pltpu.VMEM(share, jnp.bfloat16),
            pltpu.SemaphoreType.DMA((groups + 1,)),
        ],
        compiler_params=pltpu.CompilerParams(vmem_limit_bytes=40 * 2**20),
        name="anomaly",
    )(counts, tile_rows(field), tile_rows(climate), climate)


def tile_rows(array):
    *lead, hours, cells = array.shape
    tiles = cells // LANES
    split = array.reshape(-1, hours, tiles, LANES)
    split = with_layout_constraint(split, Layout(major_to_minor=(0, 2, 1, 3)))
    return split.transpose(0, 2, 1, 3).reshape(-1, LANES)


def from_tile_rows(rows, shape):
    *lead, hours, cells = shape
    tiles = cells // LANES
    split = rows.reshape(-1, tiles, hours, LANES).transpose(0, 2, 1, 3)
    split = with_layout_constraint(split, Layout(major_to_minor=(0, 2, 1, 3)))
    return split.reshape(shape)


def local(field, day_index, sample_count):
    slot = lax.broadcasted_iota(jnp.int32, sample_count.shape, 1) + lax.axis_index("day") * DAYS
    counts = jnp.where(day_index[:, :, None] != slot, -sample_count, sample_count)
    counts = jnp.transpose(counts, (0, 2, 1))
    climate, field = climate_of(field, counts)
    cells = TILES * LANES // lax.axis_size("year")
    anomaly, share = anomaly_of(field, counts, climate, cells)
    return from_tile_rows(anomaly, field.shape), share


def solution(mesh):
    return jax.shard_map(
        local,
        mesh=mesh,
        in_specs=(P("year", "day", None, None), P("year", "day"), P("year", "day", None)),
        out_specs=(P("year", "day", None, None), P("day", None, "year")),
        check_vma=False,
    )
```
